256 devices in a mesh: dp: 8 (over z), section: 2 (over core), space: 16 (over y, x).
Axes of the slice: x: 4, y: 4, z: 8, core: 2. Of those that a mesh axis runs over, the one named last changes fastest.
Arguments:
- latents: bfloat16 [32, 96, 192, 320], P('dp', 'space'), parts along dimension 0, may hold values from -16 to 16
- kernels: bfloat16 [2, 3, 3, 320, 320], P('section'), may hold values from -0.109375 to 0.109375
- norm_gain: float32 [2, 320], P('section'), may hold values from 0.25 to 1.75
- norm_bias: float32 [2, 320], P('section'), may hold values from -3 to 3
- conv_bias: float32 [2, 320], P('section'), may hold values from -3 to 3
Outputs:
- skips: bfloat16 [2, 32, 96, 192, 320], P('section', 'dp', 'space'), parts along dimension 1
The draws below stay inside these ranges and needn't reach their ends.
There are 8 independent parts, one for each index of `dp`. The reference program is written for one: setup_inputs(seed, part) draws one part's arguments, and reference() takes and returns one part's arrays. A program takes and returns all parts, laid end to end along the dimension named above; an argument that names none is the same for every part. Nothing has to cross between parts.
All inputs are finite; a program needn't handle non-finite values.
Results may differ from the reference program's by a relative error of at most 0.01.
Values may be sent and summed in bfloat16 or wider, within the bound.
No kernel may reach another device: no remote copies, remote signals or barrier semaphores. Data moves between devices by JAX's collectives and lax.ppermute only.
A program may use at most 128 MiB of HBM per device.

```python
import jax
import jax.numpy as jnp
from jax import lax

C = 320
GROUPS = 32
H = 96
W = 192
MICRO = 4
SECTIONS = 2


def draw_latents(key, part):
    noise_key = jax.random.fold_in(key, 101)
    offset_key = jax.random.fold_in(key, 202)
    positions = jnp.arange(H, dtype=jnp.float32) / (H - 1)
    base = jax.random.normal(noise_key, (MICRO, H, W, C), jnp.float32)
    scales = 0.4 * jnp.exp(jnp.log(3.0) * positions)
    ramp = 0.3 * jnp.exp(jnp.log(10.0) * positions)
    offsets = 0.6 * jax.random.normal(offset_key, (MICRO, 1, 1, C), jnp.float32) + 1.0
    values = base * scales[None, :, None, None] + offsets * ramp[None, :, None, None]
    return jnp.clip(values, -16.0, 16.0).astype(jnp.bfloat16)


def block_levels(stream_key, dims, shards, least, largest):
    level, own = 1.0, jax.random.fold_in(stream_key, 6)
    for axis_at, shards_of in shards:
        heights = jnp.exp(jax.random.uniform(jax.random.fold_in(own, axis_at), (shards_of,), jnp.float32, least / len(shards), largest / len(shards)))
        level = level * jnp.repeat(heights, dims[axis_at] // shards_of).reshape([-1 if axis == axis_at else 1 for axis in range(len(dims))])
    return level


def gaussian(key, dims, scale, reach, cuts=(), held_as=jnp.bfloat16):
    level = block_levels(key, dims, cuts, -0.22, 0.18) if cuts else 1.0
    result = jax.random.normal(key, dims, jnp.float32) * scale * level
    return jnp.minimum(jnp.maximum(result, -reach), reach).astype(held_as)


def setup_inputs(seed: int = 0, part: int = 0) -> dict:
    splits = jax.random.split(jax.random.key(seed), 6)
    own_keys = jax.random.split(jax.random.fold_in(splits[5], part), 6)
    return {
        "latents": draw_latents(jax.random.fold_in(jax.random.fold_in(splits[5], part), 71), part),
        "kernels": gaussian(splits[1], (SECTIONS, 3, 3, C, C), (9 * C) ** -0.5, 0.109375, ((0, 2),)),
        "norm_gain": jnp.clip(1.0 + 0.15 * jax.random.normal(splits[2], (SECTIONS, C), jnp.float32), 0.25, 1.75),
        "norm_bias": gaussian(splits[3], (SECTIONS, C), 0.5, 3.0, ((0, 2),), jnp.float32),
        "conv_bias": gaussian(splits[4], (SECTIONS, C), 0.5, 3.0, ((0, 2),), jnp.float32),
    }


def group_norm_silu(inputs, norm_gain, norm_shift):
    batch_count = inputs.shape[0]
    values = inputs.astype(jnp.float32).reshape(batch_count, H * W, GROUPS, C // GROUPS)
    group_mean = lax.optimization_barrier(jnp.mean(values, axis=(1, 3), keepdims=True))
    deviation = values - group_mean
    group_var = lax.optimization_barrier(jnp.mean(deviation * deviation, axis=(1, 3), keepdims=True))
    scaled = (deviation * lax.rsqrt(group_var + 1e-05)).reshape(batch_count, H, W, C)
    scaled = scaled * norm_gain + norm_shift
    return jax.nn.silu(scaled).astype(jnp.bfloat16)

def convolve(normed, kernel):
    return lax.conv_general_dilated(normed, kernel, (1, 1), ((1, 1), (1, 1)), dimension_numbers=('NHWC', 'HWIO', 'NHWC'), preferred_element_type=jnp.float32)

def reference(latents, kernels, norm_gain, norm_bias, conv_bias):
    normed_first = group_norm_silu(latents, norm_gain[0], norm_bias[0])
    first = (convolve(normed_first, kernels[0]) + conv_bias[0]).astype(jnp.bfloat16)
    normed_second = group_norm_silu(first, norm_gain[1], norm_bias[1])
    second = (latents.astype(jnp.float32) + convolve(normed_second, kernels[1]) + conv_bias[1]).astype(jnp.bfloat16)
    return jnp.stack([first, second])
```

```python
import jax
import jax.numpy as jnp
from jax import lax
from jax.experimental import pallas as pl
from jax.experimental.pallas import tpu as pltpu
from jax.sharding import PartitionSpec as P

GROUPS = 32
F32 = jnp.float32
BF16 = jnp.bfloat16
ANY = pl.BlockSpec(memory_space=pl.ANY)
VM = pl.BlockSpec(memory_space=pltpu.VMEM)


def one_hot(shape, channel_dim, per_group):
    channel = lax.broadcasted_iota(jnp.int32, shape, channel_dim)
    group = lax.broadcasted_iota(jnp.int32, shape, 1 - channel_dim)
    low = group * per_group
    return jnp.where((channel >= low) & (channel < low + per_group), 1.0, 0.0).astype(BF16)


def exact_dot(values, selector):
    high = values.astype(BF16)
    rest = values - high.astype(F32)
    middle = rest.astype(BF16)
    low = (rest - middle.astype(F32)).astype(BF16)
    return (
        jnp.dot(high, selector, preferred_element_type=F32)
        + jnp.dot(middle, selector, preferred_element_type=F32)
        + jnp.dot(low, selector, preferred_element_type=F32)
    )


def send_group_sums(sums, stats_out, per_group):
    channels = sums.shape[1]
    grouped = exact_dot(sums, one_hot((channels, 128), 0, per_group))
    for i in range(stats_out.shape[0]):
        stats_out[i] = grouped


def fold_rows(block):
    return block.reshape(block.shape[0] // 8, 8, block.shape[1]).sum(axis=0)


def stats_kernel(x_any, stats_out, ha_out, hb_out, x_buf, sem, sem_out):
    n, rows, cols, ch = x_buf.shape
    sec = lax.axis_index("section")
    even = lax.axis_index("space") % 2 == 0
    loads = []
    for s in range(n):
        cp = pltpu.make_async_copy(x_any.at[sec * n + s], x_buf.at[s], sem.at[s])
        cp.start()
        loads.append(cp)
    total = []
    row_a = jnp.where(even, rows - 1, 0)
    sends = []
    for s in range(n):
        loads[s].wait()
        for k, (dst, row) in enumerate(((ha_out, row_a), (hb_out, rows - 1 - row_a))):
            cp = pltpu.make_async_copy(x_buf.at[s, row], dst.at[s], sem_out.at[2 * s + k])
            cp.start()
            sends.append(cp)

        def step(r, carry):
            acc, sq = carry
            v = x_buf[s, r].astype(F32)
            return acc + fold_rows(v), sq + fold_rows(v * v)

        zero = jnp.zeros((8, ch), F32)
        acc, sq = lax.fori_loop(0, rows, step, (zero, zero))
        total += [acc.sum(axis=0, keepdims=True), sq.sum(axis=0, keepdims=True)]
    sums = jnp.concatenate(total + [jnp.zeros((8 - len(total), ch), F32)], axis=0)
    send_group_sums(sums, stats_out, ch // GROUPS)
    for cp in sends:
        cp.wait()


def weight_kernel(own_ref, other_ref, w0_ref, w1_ref):
    sec = lax.axis_index("section")

    def lay_out(src, dst):
        ch = src.shape[-1]
        rem = ch - 256
        for dr in range(3):
            for dc in range(3):
                dst[dr * 256 : dr * 256 + 256, dc * 256 : dc * 256 + 256] = src[0, dr, dc, 0:256, 0:256]
                dst[768 + dr * rem : 768 + dr * rem + rem, dc * 256 : dc * 256 + 256] = src[
                    0, dr, dc, 256:ch, 0:256
                ]
            right = [src[0, dr, dc, :, 256:ch].astype(F32) for dc in range(3)]
            right = jnp.concatenate(right + [jnp.zeros((ch, 256 - 3 * rem), F32)], axis=1).astype(BF16)
            dst[dr * 256 : dr * 256 + 256, 768:1024] = right[0:256]
            dst[768 + dr * rem : 768 + dr * rem + rem, 768:1024] = right[256:ch]
        dst[768 + 3 * rem : 1024, :] = jnp.zeros((256 - 3 * rem, 1024), BF16)

    @pl.when(sec == 0)
    def _():
        lay_out(own_ref, w0_ref)
        lay_out(other_ref, w1_ref)

    @pl.when(sec != 0)
    def _():
        lay_out(other_ref, w0_ref)
        lay_out(own_ref, w1_ref)


def conv_kernel(index, members, n_space, chunk_rows, *refs):
    if index == 0:
        (x_any, ra_any, rb_any, stats_ref, own_p, other_p, w_ref,
         y_out, stats_out, ha_out, hb_out,
         x_buf, xm, xr, rem_buf, z_buf, y_buf, sem) = refs
    else:
        (x_any, ra_any, rb_any, stats_ref, own_p, other_p, w_ref, lat_any, first_other,
         y_out, full_out,
         x_buf, xm, xr, rem_buf, z_buf, y_buf, lat_buf, sem) = refs
    n, padded_rows, cols, ch = x_buf.shape
    rows = padded_rows - 2
    rem = ch - 256
    sec = lax.axis_index("section")
    space = lax.axis_index("space")
    even = space % 2 == 0
    slot_a = jnp.where(even, rows + 1, 0)
    loads = []
    for s in range(n):
        src = x_any.at[sec * n + s] if index == 0 else x_any.at[s]
        group = [
            pltpu.make_async_copy(ra_any.at[s], x_buf.at[s, slot_a], sem.at[0, s]),
            pltpu.make_async_copy(rb_any.at[s], x_buf.at[s, rows + 1 - slot_a], sem.at[1, s]),
            pltpu.make_async_copy(src, x_buf.at[s, pl.ds(1, rows)], sem.at[2, s]),
        ]
        if index == 1:
            group.append(pltpu.make_async_copy(lat_any.at[sec * n + s], lat_buf.at[s], sem.at[3, s]))
        for cp in group:
            cp.start()
        loads.append(group)
    if index == 1:
        keep_own = pltpu.make_async_copy(x_any, full_out.at[pl.ds(0, n)], sem.at[5, 0])
        keep_other = pltpu.make_async_copy(first_other, full_out.at[pl.ds(n, n)], sem.at[5, 1])

        @pl.when(sec == 0)
        def _():
            keep_own.start()
            keep_other.start()

    params = jnp.where(sec == index, own_p[...], other_p[...])
    gain, shift, bias = params[0:1], params[1:2], params[2:3]
    total = stats_ref[0]
    for i in range(1, n_space):
        total = total + stats_ref[i]
    packed = []
    for s in range(n):
        mean = total[2 * s : 2 * s + 1] * (1.0 / members)
        var = jnp.maximum(total[2 * s + 1 : 2 * s + 2] * (1.0 / members) - mean * mean, 0.0)
        packed += [mean, lax.rsqrt(var + 1e-05)]
    packed = jnp.concatenate(packed + [jnp.zeros((8 - 2 * n, 128), F32)], axis=0)
    spread = exact_dot(packed, one_hot((128, ch), 1, ch // GROUPS))

    if index == 0:
        acc = [[jnp.zeros((8, ch), F32) for _ in range(2)] for _ in range(n)]
    stores = []
    for s in range(n):
        for cp in loads[s]:
            cp.wait()
        half_a = 0.5 * (spread[2 * s + 1 : 2 * s + 2] * gain)
        half_b = 0.5 * shift - spread[2 * s : 2 * s + 1] * half_a
        for j in range(padded_rows):
            half = x_buf[s, j].astype(F32) * half_a + half_b
            y = half + half * jnp.tanh(half)
            if j == 0:
                y = jnp.where(space == 0, 0.0, y)
            if j == padded_rows - 1:
                y = jnp.where(space == n_space - 1, 0.0, y)
            xm[s, pl.ds(j * cols, cols), :] = y[:, 0:256].astype(BF16)
            rem_buf[j] = y[:, 256:ch]
            if j >= 2:
                parts = [rem_buf[j - 2], rem_buf[j - 1], rem_buf[j], jnp.zeros((cols, 256 - 3 * rem), F32)]
                xr[s, pl.ds((j - 2) * cols, cols), :] = jnp.concatenate(parts, axis=1).astype(BF16)
        for r0 in range(0, rows, chunk_rows):
            m = chunk_rows * cols
            lhs = jnp.concatenate(
                [xm[s, pl.ds((r0 + dr) * cols, m), :] for dr in range(3)] + [xr[s, pl.ds(r0 * cols, m), :]],
                axis=1,
            )
            slot = (r0 // chunk_rows) % 2
            z_buf[slot] = jnp.dot(lhs, w_ref[...], preferred_element_type=F32)
            first_slab = lax.broadcasted_iota(jnp.int32, (8, 256), 0) == 0
            last_slab = lax.broadcasted_iota(jnp.int32, (8, 256), 0) == 7
            for r in range(chunk_rows):
                at = pl.ds(r * cols, cols)

                def down(z, width):
                    moved = pltpu.roll(z, 1, 0)
                    head = jnp.where(first_slab[:, :width], 0.0, moved[0:8])
                    return jnp.concatenate([head, moved[8:]], axis=0)

                def up(z, width):
                    moved = pltpu.roll(z, cols - 1, 0)
                    tail = jnp.where(last_slab[:, :width], 0.0, moved[cols - 8 :])
                    return jnp.concatenate([moved[: cols - 8], tail], axis=0)

                main = z_buf[slot, at, 256:512] + down(z_buf[slot, at, 0:256], 256) + up(z_buf[slot, at, 512:768], 256)
                left = z_buf[slot, at, 768:896]
                right = z_buf[slot, at, 896:1024]
                side = down(left, 128) + pltpu.roll(left, 64, 1) + up(right, 128)
                out = jnp.concatenate([main, side[:, 0:rem]], axis=1) + bias
                if index == 1:
                    out = out + lat_buf[s, r0 + r].astype(F32)
                rounded = out.astype(BF16)
                y_buf[s, r0 + r] = rounded
                if index == 0:
                    back = rounded.astype(F32)
                    acc[s][0] = acc[s][0] + fold_rows(back)
                    acc[s][1] = acc[s][1] + fold_rows(back * back)
        cp = pltpu.make_async_copy(y_buf.at[s], y_out.at[s], sem.at[4, s])
        cp.start()
        stores.append(cp)
        if index == 0:
            for k, (dst, row) in enumerate(((ha_out, slot_a), (hb_out, rows + 1 - slot_a))):
                cp = pltpu.make_async_copy(
                    y_buf.at[s, jnp.clip(row - 1, 0, rows - 1)], dst.at[s], sem.at[5 + k, s]
                )
                cp.start()
                stores.append(cp)
        else:
            keep_new = pltpu.make_async_copy(y_buf.at[s], full_out.at[n + s], sem.at[6, s])

            @pl.when(sec != 0)
            def _():
                keep_new.start()

    if index == 0:
        rows_out = []
        for s in range(n):
            rows_out += [v.sum(axis=0, keepdims=True) for v in acc[s]]
        sums = jnp.concatenate(rows_out + [jnp.zeros((8 - 2 * n, ch), F32)], axis=0)
        send_group_sums(sums, stats_out, ch // GROUPS)
    for cp in stores:
        cp.wait()
    if index == 1:

        @pl.when(sec == 0)
        def _():
            keep_own.wait()
            keep_other.wait()

        @pl.when(sec != 0)
        def _():
            for s in range(n):
                pltpu.make_async_copy(y_buf.at[s], full_out.at[n + s], sem.at[6, s]).wait()


def finish_kernel(full_in, second_other, full_out, sem):
    n = second_other.shape[0]
    cp = pltpu.make_async_copy(second_other, full_out.at[pl.ds(0, n)], sem)

    @pl.when(lax.axis_index("section") != 0)
    def _():
        cp.start()
        cp.wait()


def swap(array):
    return lax.ppermute(array, "section", [(0, 1), (1, 0)])


def on_device(latents, kernels, norm_gain, norm_bias, conv_bias):
    samples, rows, cols, ch = latents.shape
    n = samples // lax.axis_size("section")
    n_space = lax.axis_size("space")
    members = rows * n_space * cols * (ch // GROUPS)
    pairs_a = [(i, i ^ 1) for i in range(n_space)]
    pairs_b = [(i, (i - 1) % n_space if i % 2 == 0 else (i + 1) % n_space) for i in range(n_space)]
    shape = jax.ShapeDtypeStruct
    stats_shape = shape((n_space, 8, 128), F32)
    edge_shape = shape((n, cols, ch), BF16)
    part_shape = shape((n, rows, cols, ch), BF16)
    limit = pltpu.CompilerParams(vmem_limit_bytes=40 * 1024 * 1024)

    own_p = jnp.concatenate([norm_gain, norm_bias, conv_bias], axis=0)
    other_p = swap(own_p)
    other_k = swap(kernels)

    stats, ha, hb = pl.pallas_call(
        stats_kernel,
        out_shape=(stats_shape, edge_shape, edge_shape),
        in_specs=[ANY],
        out_specs=(VM, ANY, ANY),
        scratch_shapes=[
            pltpu.VMEM((n, rows, cols, ch), BF16),
            pltpu.SemaphoreType.DMA((n,)),
            pltpu.SemaphoreType.DMA((2 * n,)),
        ],
        compiler_params=limit,
        name="stats",
    )(latents)
    ra = lax.ppermute(ha, "space", pairs_a)
    rb = lax.ppermute(hb, "space", pairs_b)
    stats = lax.all_to_all(stats, "space", split_axis=0, concat_axis=0, tiled=True)

    w_shape = shape((1024, 1024), BF16)
    w0, w1 = pl.pallas_call(
        weight_kernel,
        out_shape=(w_shape, w_shape),
        in_specs=[VM, VM],
        out_specs=(VM, VM),
        compiler_params=limit,
        name="weights",
    )(kernels, other_k)

    chunk_rows = 2

    def conv(index, operands, out_shape, out_specs, extra):
        body = lambda *refs: conv_kernel(index, members, n_space, chunk_rows, *refs)
        return pl.pallas_call(
            body,
            out_shape=out_shape,
            in_specs=[ANY, ANY, ANY, VM, VM, VM, VM] + [ANY] * (len(operands) - 7),
            out_specs=out_specs,
            scratch_shapes=[
                pltpu.VMEM((n, rows + 2, cols, ch), BF16),
                pltpu.VMEM((n, (rows + 2) * cols, 256), BF16),
                pltpu.VMEM((n, rows * cols, 256), BF16),
                pltpu.VMEM((rows + 2, cols, ch - 256), F32),
                pltpu.VMEM((2, chunk_rows * cols, 1024), F32),
                pltpu.VMEM((n, rows, cols, ch), BF16),
                *extra,
                pltpu.SemaphoreType.DMA((7, n)),
            ],
            compiler_params=limit,
            name="conv%d" % index,
        )(*operands)

    first, stats, ha, hb = conv(
        0,
        (latents, ra, rb, stats, own_p, other_p, w0),
        (part_shape, stats_shape, edge_shape, edge_shape),
        (ANY, VM, ANY, ANY),
        (),
    )
    ra = lax.ppermute(ha, "space", pairs_a)
    rb = lax.ppermute(hb, "space", pairs_b)
    first_other = swap(first)
    stats = lax.all_to_all(stats, "space", split_axis=0, concat_axis=0, tiled=True)
    full_shape = shape((samples, rows, cols, ch), BF16)
    second, full = conv(
        1,
        (first, ra, rb, stats, own_p, other_p, w1, latents, first_other),
        (part_shape, full_shape),
        (ANY, ANY),
        (pltpu.VMEM((n, rows, cols, ch), BF16),),
    )
    second_other = swap(second)
    full = pl.pallas_call(
        finish_kernel,
        out_shape=full_shape,
        in_specs=[ANY, ANY],
        out_specs=ANY,
        scratch_shapes=[pltpu.SemaphoreType.DMA],
        input_output_aliases={0: 0},
        name="finish",
    )(full, second_other)
    return full[None]


def solution(mesh):
    return jax.shard_map(
        on_device,
        mesh=mesh,
        in_specs=(
            P("dp", "space", None, None),
            P("section", None, None, None, None),
            P("section", None),
            P("section", None),
            P("section", None),
        ),
        out_specs=P("section", "dp", "space", None, None),
        check_vma=False,
    )
```

```python
import jax
import jax.numpy as jnp
from jax import lax
from jax.experimental import pallas as pl
from jax.experimental.pallas import tpu as pltpu
from jax.sharding import PartitionSpec as P

GROUPS = 32
F32 = jnp.float32
BF16 = jnp.bfloat16
ANY = pl.BlockSpec(memory_space=pl.ANY)
VM = pl.BlockSpec(memory_space=pltpu.VMEM)
HBM = pl.BlockSpec(memory_space=pltpu.HBM)


def one_hot(shape, channel_dim, per_group):
    channel = lax.broadcasted_iota(jnp.int32, shape, channel_dim)
    group = lax.broadcasted_iota(jnp.int32, shape, 1 - channel_dim)
    low = group * per_group
    return jnp.where((channel >= low) & (channel < low + per_group), 1.0, 0.0).astype(BF16)


def exact_dot(values, selector):
    high = values.astype(BF16)
    rest = values - high.astype(F32)
    middle = rest.astype(BF16)
    low = (rest - middle.astype(F32)).astype(BF16)
    return (
        jnp.dot(high, selector, preferred_element_type=F32)
        + jnp.dot(middle, selector, preferred_element_type=F32)
        + jnp.dot(low, selector, preferred_element_type=F32)
    )


def send_group_sums(sums, stats_out, per_group):
    channels = sums.shape[1]
    grouped = exact_dot(sums, one_hot((channels, 128), 0, per_group))
    for i in range(stats_out.shape[0]):
        stats_out[i] = grouped


def fold_rows(block):
    return block.reshape(block.shape[0] // 8, 8, block.shape[1]).sum(axis=0)


def stats_kernel(x_any, stats_out, ha_out, hb_out, x_buf, sem):
    n, rows, cols, ch = x_buf.shape
    sec = lax.axis_index("section")
    even = lax.axis_index("space") % 2 == 0
    loads = []
    for s in range(n):
        cp = pltpu.make_async_copy(x_any.at[sec * n + s], x_buf.at[s], sem.at[s])
        cp.start()
        loads.append(cp)
    total = []
    row_a = jnp.where(even, rows - 1, 0)
    for s in range(n):
        loads[s].wait()
        ha_out[s] = x_buf[s, row_a]
        hb_out[s] = x_buf[s, rows - 1 - row_a]

        def step(r, carry):
            acc, sq = carry
            v = x_buf[s, r].astype(F32)
            return acc + fold_rows(v), sq + fold_rows(v * v)

        zero = jnp.zeros((8, ch), F32)
        acc, sq = lax.fori_loop(0, rows, step, (zero, zero))
        total += [acc.sum(axis=0, keepdims=True), sq.sum(axis=0, keepdims=True)]
    sums = jnp.concatenate(total + [jnp.zeros((8 - len(total), ch), F32)], axis=0)
    send_group_sums(sums, stats_out, ch // GROUPS)


def lay_out_right(src, right_ref):
    ch = src.shape[-1]
    rem = ch - 256
    for dr in range(3):
        right = [src[0, dr, dc, :, 256:ch].astype(F32) for dc in range(3)]
        right = jnp.concatenate(right + [jnp.zeros((ch, 256 - 3 * rem), F32)], axis=1).astype(BF16)
        right_ref[dr * 256 : dr * 256 + 256, :] = right[0:256]
        right_ref[768 + dr * rem : 768 + dr * rem + rem, :] = right[256:ch]
    right_ref[768 + 3 * rem : 1024, :] = jnp.zeros((256 - 3 * rem, 256), BF16)


def kernel_columns(src, dc):
    ch = src.shape[-1]
    parts = [src[0, dr, dc, 0:256, 0:256] for dr in range(3)] + [src[0, dr, dc, 256:ch, 0:256] for dr in range(3)]
    return jnp.concatenate(parts + [jnp.zeros((1024 - 3 * ch, 256), BF16)], axis=0)


def conv_kernel(index, members, n_space, chunk_rows, *refs):
    if index == 0:
        (lat_hbm, ra_ref, rb_ref, stats_ref, own_p, other_p, own_k, other_k,
         y_out, stats_out, ha_out, hb_out,
         lat_buf, w_buf, right_buf, xm, xr, rem_buf, z_buf, sem) = refs
        x_ref = lat_buf
    else:
        (lat_hbm, ra_ref, rb_ref, stats_ref, own_p, other_p, own_k, other_k, x_ref, first_other,
         y_out, full_out,
         lat_buf, w_buf, right_buf, xm, xr, rem_buf, z_buf, sem) = refs
    n, rows, cols, ch = lat_buf.shape
    padded_rows = rows + 2
    rem = ch - 256
    sec = lax.axis_index("section")
    space = lax.axis_index("space")
    even = space % 2 == 0
    lat_loads = [
        pltpu.make_async_copy(lat_hbm.at[sec * n + s], lat_buf.at[s], sem.at[2, s]) for s in range(n)
    ]
    if index == 0:
        for cp in lat_loads:
            cp.start()

    @pl.when(sec == index)
    def _():
        pltpu.make_async_copy(own_k, w_buf, sem.at[3, 0]).start()

    @pl.when(sec != index)
    def _():
        pltpu.make_async_copy(other_k, w_buf, sem.at[3, 0]).start()

    if index == 1:
        for cp in lat_loads:
            cp.start()
    if index == 1:
        keep_own = pltpu.make_async_copy(x_ref, full_out.at[pl.ds(0, n)], sem.at[0, 0])
        keep_other = pltpu.make_async_copy(first_other, full_out.at[pl.ds(n, n)], sem.at[0, 1])

        @pl.when(sec == 0)
        def _():
            keep_own.start()
            keep_other.start()

    params = jnp.where(sec == index, own_p[...], other_p[...])
    gain, shift, bias = params[0:1], params[1:2], params[2:3]
    total = stats_ref[0]
    for i in range(1, n_space):
        total = total + stats_ref[i]
    packed = []
    for s in range(n):
        mean = total[2 * s : 2 * s + 1] * (1.0 / members)
        var = jnp.maximum(total[2 * s + 1 : 2 * s + 2] * (1.0 / members) - mean * mean, 0.0)
        packed += [mean, lax.rsqrt(var + 1e-05)]
    packed = jnp.concatenate(packed + [jnp.zeros((8 - 2 * n, 128), F32)], axis=0)
    spread = exact_dot(packed, one_hot((128, ch), 1, ch // GROUPS))

    if index == 0:
        acc = [[jnp.zeros((8, ch), F32) for _ in range(2)] for _ in range(n)]
    row_a = jnp.where(even, rows - 1, 0)
    for s in range(n):
        if index == 0:
            lat_loads[s].wait()
        half_a = 0.5 * (spread[2 * s + 1 : 2 * s + 2] * gain)
        half_b = 0.5 * shift - spread[2 * s : 2 * s + 1] * half_a
        for j in range(padded_rows):
            if j == 0:
                source = jnp.where(even, rb_ref[s], ra_ref[s])
            elif j == padded_rows - 1:
                source = jnp.where(even, ra_ref[s], rb_ref[s])
            else:
                source = x_ref[s, j - 1]
            half = source.astype(F32) * half_a + half_b
            y = half + half * jnp.tanh(half)
            if j == 0:
                y = jnp.where(space == 0, 0.0, y)
            if j == padded_rows - 1:
                y = jnp.where(space == n_space - 1, 0.0, y)
            xm[s, pl.ds(j * cols, cols), :] = y[:, 0:256].astype(BF16)
            rem_buf[j] = y[:, 256:ch]
            if j >= 2:
                parts = [rem_buf[j - 2], rem_buf[j - 1], rem_buf[j], jnp.zeros((cols, 256 - 3 * rem), F32)]
                xr[s, pl.ds((j - 2) * cols, cols), :] = jnp.concatenate(parts, axis=1).astype(BF16)
        if s == 0:
            pltpu.make_async_copy(own_k, w_buf, sem.at[3, 0]).wait()
            lay_out_right(w_buf, right_buf)
        if index == 1:
            lat_loads[s].wait()
        for r0 in range(0, rows, chunk_rows):
            m = chunk_rows * cols
            lhs = jnp.concatenate(
                [xm[s, pl.ds((r0 + dr) * cols, m), :] for dr in range(3)] + [xr[s, pl.ds(r0 * cols, m), :]],
                axis=1,
            )
            slot = (r0 // chunk_rows) % 2
            for dc in range(3):
                z_buf[slot, :, dc * 256 : dc * 256 + 256] = jnp.dot(
                    lhs, kernel_columns(w_buf, dc), preferred_element_type=F32
                )
            z_buf[slot, :, 768:1024] = jnp.dot(lhs, right_buf[...], preferred_element_type=F32)
            first_slab = lax.broadcasted_iota(jnp.int32, (8, 256), 0) == 0
            last_slab = lax.broadcasted_iota(jnp.int32, (8, 256), 0) == 7
            for r in range(chunk_rows):
                at = pl.ds(r * cols, cols)

                def down(z, width):
                    moved = pltpu.roll(z, 1, 0)
                    head = jnp.where(first_slab[:, :width], 0.0, moved[0:8])
                    return jnp.concatenate([head, moved[8:]], axis=0)

                def up(z, width):
                    moved = pltpu.roll(z, cols - 1, 0)
                    tail = jnp.where(last_slab[:, :width], 0.0, moved[cols - 8 :])
                    return jnp.concatenate([moved[: cols - 8], tail], axis=0)

                main = z_buf[slot, at, 256:512] + down(z_buf[slot, at, 0:256], 256) + up(z_buf[slot, at, 512:768], 256)
                left = z_buf[slot, at, 768:896]
                right = z_buf[slot, at, 896:1024]
                side = down(left, 128) + pltpu.roll(left, 64, 1) + up(right, 128)
                out = jnp.concatenate([main, side[:, 0:rem]], axis=1) + bias
                if index == 1:
                    out = out + lat_buf[s, r0 + r].astype(F32)
                rounded = out.astype(BF16)
                y_out[s, r0 + r] = rounded
                if index == 0:
                    back = rounded.astype(F32)
                    acc[s][0] = acc[s][0] + fold_rows(back)
                    acc[s][1] = acc[s][1] + fold_rows(back * back)
        if index == 0:
            ha_out[s] = y_out[s, row_a]
            hb_out[s] = y_out[s, rows - 1 - row_a]
        else:
            keep_new = pltpu.make_async_copy(y_out.at[s], full_out.at[n + s], sem.at[1, s])

            @pl.when(sec != 0)
            def _():
                keep_new.start()

    if index == 0:
        rows_out = []
        for s in range(n):
            rows_out += [v.sum(axis=0, keepdims=True) for v in acc[s]]
        sums = jnp.concatenate(rows_out + [jnp.zeros((8 - 2 * n, ch), F32)], axis=0)
        send_group_sums(sums, stats_out, ch // GROUPS)
    if index == 1:

        @pl.when(sec == 0)
        def _():
            keep_own.wait()
            keep_other.wait()

        @pl.when(sec != 0)
        def _():
            for s in range(n):
                pltpu.make_async_copy(y_out.at[s], full_out.at[n + s], sem.at[1, s]).wait()


def finish_kernel(full_in, second_other, full_out, sem):
    n = second_other.shape[0]
    cp = pltpu.make_async_copy(second_other, full_out.at[pl.ds(0, n)], sem)

    @pl.when(lax.axis_index("section") != 0)
    def _():
        cp.start()
        cp.wait()


def swap(array):
    return lax.ppermute(array, "section", [(0, 1), (1, 0)])


def on_device(latents, kernels, norm_gain, norm_bias, conv_bias):
    samples, rows, cols, ch = latents.shape
    n = samples // lax.axis_size("section")
    n_space = lax.axis_size("space")
    members = rows * n_space * cols * (ch // GROUPS)
    pairs_a = [(i, i ^ 1) for i in range(n_space)]
    pairs_b = [(i, (i - 1) % n_space if i % 2 == 0 else (i + 1) % n_space) for i in range(n_space)]
    shape = jax.ShapeDtypeStruct
    stats_shape = shape((n_space, 8, 128), F32)
    edge_shape = shape((n, cols, ch), BF16)
    part_shape = shape((n, rows, cols, ch), BF16)
    limit = pltpu.CompilerParams(vmem_limit_bytes=32 * 1024 * 1024)

    latents = pltpu.with_memory_space_constraint(latents, pltpu.HBM)
    kernels = pltpu.with_memory_space_constraint(kernels, pltpu.HBM)
    own_p = jnp.concatenate([norm_gain, norm_bias, conv_bias], axis=0)
    other_p = swap(own_p)
    other_k = pltpu.with_memory_space_constraint(swap(kernels), pltpu.HBM)

    stats, ha, hb = pl.pallas_call(
        stats_kernel,
        out_shape=(stats_shape, edge_shape, edge_shape),
        in_specs=[HBM],
        out_specs=(VM, VM, VM),
        scratch_shapes=[
            pltpu.VMEM((n, rows, cols, ch), BF16),
            pltpu.SemaphoreType.DMA((n,)),
        ],
        compiler_params=limit,
        name="stats",
    )(latents)
    ra = lax.ppermute(ha, "space", pairs_a)
    rb = lax.ppermute(hb, "space", pairs_b)
    stats = lax.all_to_all(stats, "space", split_axis=0, concat_axis=0, tiled=True)

    chunk_rows = 2

    def conv(index, operands, out_shape, out_specs):
        body = lambda *refs: conv_kernel(index, members, n_space, chunk_rows, *refs)
        return pl.pallas_call(
            body,
            out_shape=out_shape,
            in_specs=[HBM, VM, VM, VM, VM, VM, HBM, HBM] + [VM] * (len(operands) - 8),
            out_specs=out_specs,
            scratch_shapes=[
                pltpu.VMEM((n, rows, cols, ch), BF16),
                pltpu.VMEM(kernels.shape, BF16),
                pltpu.VMEM((1024, 256), BF16),
                pltpu.VMEM((n, (rows + 2) * cols, 256), BF16),
                pltpu.VMEM((n, rows * cols, 256), BF16),
                pltpu.VMEM((rows + 2, cols, ch - 256), F32),
                pltpu.VMEM((2, chunk_rows * cols, 1024), F32),
                pltpu.SemaphoreType.DMA((4, n)),
            ],
            compiler_params=limit,
            name="conv%d" % index,
        )(*operands)

    first, stats, ha, hb = conv(
        0,
        (latents, ra, rb, stats, own_p, other_p, kernels, other_k),
        (part_shape, stats_shape, edge_shape, edge_shape),
        (VM, VM, VM, VM),
    )
    ra = lax.ppermute(ha, "space", pairs_a)
    rb = lax.ppermute(hb, "space", pairs_b)
    first_other = swap(first)
    stats = lax.all_to_all(stats, "space", split_axis=0, concat_axis=0, tiled=True)
    full_shape = shape((samples, rows, cols, ch), BF16)
    second, full = conv(
        1,
        (latents, ra, rb, stats, own_p, other_p, kernels, other_k, first, first_other),
        (part_shape, full_shape),
        (VM, HBM),
    )
    second_other = swap(second)
    full = pl.pallas_call(
        finish_kernel,
        out_shape=full_shape,
        in_specs=[HBM, VM],
        out_specs=HBM,
        scratch_shapes=[pltpu.SemaphoreType.DMA],
        input_output_aliases={0: 0},
        compiler_params=pltpu.CompilerParams(vmem_limit_bytes=1024 * 1024),
        name="finish",
    )(full, second_other)
    return full[None]


def solution(mesh):
    return jax.shard_map(
        on_device,
        mesh=mesh,
        in_specs=(
            P("dp", "space", None, None),
            P("section", None, None, None, None),
            P("section", None),
            P("section", None),
            P("section", None),
        ),
        out_specs=P("section", "dp", "space", None, None),
        check_vma=False,
    )
```

```python
import jax
import jax.numpy as jnp
from jax import lax
from jax.experimental import pallas as pl
from jax.experimental.pallas import tpu as pltpu
from jax.sharding import PartitionSpec as P

GROUPS = 32
HEAD = 5
EARLY = (2, 6)
CHUNKS = ((2, 2, 2), (2, 2, 2))
F32 = jnp.float32
BF16 = jnp.bfloat16
ANY = pl.BlockSpec(memory_space=pl.ANY)
VM = pl.BlockSpec(memory_space=pltpu.VMEM)
HBM = pl.BlockSpec(memory_space=pltpu.HBM)


def one_hot(shape, channel_dim, per_group):
    channel = lax.broadcasted_iota(jnp.int32, shape, channel_dim)
    group = lax.broadcasted_iota(jnp.int32, shape, 1 - channel_dim)
    low = group * per_group
    return jnp.where((channel >= low) & (channel < low + per_group), 1.0, 0.0).astype(BF16)


def exact_dot(values, selector):
    high = values.astype(BF16)
    rest = values - high.astype(F32)
    middle = rest.astype(BF16)
    low = (rest - middle.astype(F32)).astype(BF16)
    return (
        jnp.dot(high, selector, preferred_element_type=F32)
        + jnp.dot(middle, selector, preferred_element_type=F32)
        + jnp.dot(low, selector, preferred_element_type=F32)
    )


def send_group_sums(sums, stats_out, per_group):
    channels = sums.shape[1]
    grouped = exact_dot(sums, one_hot((channels, 128), 0, per_group))
    for i in range(stats_out.shape[0]):
        stats_out[i] = grouped


def fold_rows(block):
    return block.reshape(block.shape[0] // 8, 8, block.shape[1]).sum(axis=0)


def stats_kernel(x_any, stats_out, ha_out, hb_out, x_buf, sem):
    n, rows, cols, ch = x_buf.shape
    sec = lax.axis_index("section")
    even = lax.axis_index("space") % 2 == 0
    loads = []
    for s in range(n):
        cp = pltpu.make_async_copy(x_any.at[sec * n + s], x_buf.at[s], sem.at[s])
        cp.start()
        loads.append(cp)
    total = []
    row_a = jnp.where(even, rows - 1, 0)
    for s in range(n):
        loads[s].wait()
        ha_out[s] = x_buf[s, row_a]
        hb_out[s] = x_buf[s, rows - 1 - row_a]

        def step(r, carry):
            acc, sq = carry
            v = x_buf[s, r].astype(F32)
            return acc + fold_rows(v), sq + fold_rows(v * v)

        zero = jnp.zeros((8, ch), F32)
        acc, sq = lax.fori_loop(0, rows, step, (zero, zero))
        total += [acc.sum(axis=0, keepdims=True), sq.sum(axis=0, keepdims=True)]
    sums = jnp.concatenate(total + [jnp.zeros((8 - len(total), ch), F32)], axis=0)
    send_group_sums(sums, stats_out, ch // GROUPS)


def lay_out(src, k, dst):
    ch = src.shape[-1]
    rem = ch - 256
    for dr in range(3):
        for dc in range(3):
            dst[dr * 256 : dr * 256 + 256, dc * 256 : dc * 256 + 256] = src[k, dr, dc, 0:256, 0:256]
            dst[768 + dr * rem : 768 + dr * rem + rem, dc * 256 : dc * 256 + 256] = src[k, dr, dc, 256:ch, 0:256]
        right = [src[k, dr, dc, :, 256:ch].astype(F32) for dc in range(3)]
        right = jnp.concatenate(right + [jnp.zeros((ch, 256 - 3 * rem), F32)], axis=1).astype(BF16)
        dst[dr * 256 : dr * 256 + 256, 768:1024] = right[0:256]
        dst[768 + dr * rem : 768 + dr * rem + rem, 768:1024] = right[256:ch]
    dst[768 + 3 * rem : 1024, :] = jnp.zeros((256 - 3 * rem, 1024), BF16)


def load_kernel(index, own_k, other_k, dst, sem):
    sec = lax.axis_index("section")

    @pl.when(sec == index)
    def _():
        pltpu.make_async_copy(own_k, dst, sem).start()

    @pl.when(sec != index)
    def _():
        pltpu.make_async_copy(other_k, dst, sem).start()

    return pltpu.make_async_copy(own_k, dst, sem)


def prepare_kernel(own_k, other_k, x_hbm, head_out, w_out, src, sem):
    head = head_out.shape[0]
    kernel_load = load_kernel(0, own_k, other_k, src, sem.at[0])
    at = lax.axis_index("section") * (x_hbm.shape[0] // 2)
    load = pltpu.make_async_copy(x_hbm.at[at, pl.ds(0, head)], head_out, sem.at[1])
    load.start()
    kernel_load.wait()
    lay_out(src, 0, w_out)
    load.wait()


def conv_kernel(index, members, n_space, chunks, *refs):
    if index == 0:
        (ra_ref, rb_ref, stats_ref, own_p, other_p, head_ref, w_ref, lat_hbm,
         y_out, stats_out, ha_out, hb_out,
         xm, xr, rem_buf, z_buf, lat_buf, sem) = refs
        head = head_ref.shape[0]
        loads = []
    else:
        (ra_ref, rb_ref, stats_ref, own_p, other_p, x_ref, own_k, other_k, lat_hbm,
         send_out, keep_out,
         xm, xr, rem_buf, z_buf, lat_buf, sem, w_ref, src) = refs
        head = 0
        kernel_load = load_kernel(1, own_k, other_k, src, sem.at[2])
        loads = []
    n, rows, cols, ch = lat_buf.shape
    padded_rows = rows + 2
    rem = ch - 256
    sec = lax.axis_index("section")
    space = lax.axis_index("space")
    even = space % 2 == 0
    for s in range(n):
        low = head if s == 0 else 0
        loads.append(
            pltpu.make_async_copy(
                lat_hbm.at[sec * n + s, pl.ds(low, rows - low)], lat_buf.at[s, pl.ds(low, rows - low)], sem.at[s]
            )
        )
    for cp in loads:
        cp.start()

    def source_row(s, r):
        if index == 1:
            return x_ref[s, r]
        if s == 0 and r < head:
            return head_ref[r]
        return lat_buf[s, r]

    params = jnp.where(sec == index, own_p[...], other_p[...])
    gain, shift, bias = params[0:1], params[1:2], params[2:3]
    total = stats_ref[0]
    for i in range(1, n_space):
        total = total + stats_ref[i]
    packed = []
    for s in range(n):
        mean = total[2 * s : 2 * s + 1] * (1.0 / members)
        var = jnp.maximum(total[2 * s + 1 : 2 * s + 2] * (1.0 / members) - mean * mean, 0.0)
        packed += [mean, lax.rsqrt(var + 1e-05)]
    packed = jnp.concatenate(packed + [jnp.zeros((8 - 2 * n, 128), F32)], axis=0)
    spread = exact_dot(packed, one_hot((128, ch), 1, ch // GROUPS))
    half_a = [0.5 * (spread[2 * s + 1 : 2 * s + 2] * gain) for s in range(n)]
    half_b = [0.5 * shift - spread[2 * s : 2 * s + 1] * half_a[s] for s in range(n)]

    def normalize(s, j):
        if j == 0:
            source = jnp.where(even, rb_ref[s], ra_ref[s])
        elif j == padded_rows - 1:
            source = jnp.where(even, ra_ref[s], rb_ref[s])
        else:
            source = source_row(s, j - 1)
        half = source.astype(F32) * half_a[s] + half_b[s]
        y = half + half * jnp.tanh(half)
        if j == 0:
            y = jnp.where(space == 0, 0.0, y)
        if j == padded_rows - 1:
            y = jnp.where(space == n_space - 1, 0.0, y)
        xm[s, pl.ds(j * cols, cols), :] = y[:, 0:256].astype(BF16)
        rem_buf[s, j] = y[:, 256:ch]
        if j >= 2:
            parts = [rem_buf[s, j - 2], rem_buf[s, j - 1], rem_buf[s, j], jnp.zeros((cols, 256 - 3 * rem), F32)]
            xr[s, pl.ds((j - 2) * cols, cols), :] = jnp.concatenate(parts, axis=1).astype(BF16)

    def multiply(s, r0, count, slot):
        m = count * cols
        lhs = jnp.concatenate(
            [xm[s, pl.ds((r0 + dr) * cols, m), :] for dr in range(3)] + [xr[s, pl.ds(r0 * cols, m), :]],
            axis=1,
        )
        z_buf[slot, 0:m, :] = jnp.dot(lhs, w_ref[...], preferred_element_type=F32)

    first_slab = lax.broadcasted_iota(jnp.int32, (8, 256), 0) == 0
    last_slab = lax.broadcasted_iota(jnp.int32, (8, 256), 0) == 7

    def down(z, width):
        moved = pltpu.roll(z, 1, 0)
        head = jnp.where(first_slab[:, :width], 0.0, moved[0:8])
        return jnp.concatenate([head, moved[8:]], axis=0)

    def up(z, width):
        moved = pltpu.roll(z, cols - 1, 0)
        tail = jnp.where(last_slab[:, :width], 0.0, moved[cols - 8 :])
        return jnp.concatenate([moved[: cols - 8], tail], axis=0)

    acc = [[jnp.zeros((8, ch), F32) for _ in range(2)] for _ in range(n)]

    def finish_row(s, r, slot, at):
        at = pl.ds(at * cols, cols)
        main = z_buf[slot, at, 256:512] + down(z_buf[slot, at, 0:256], 256) + up(z_buf[slot, at, 512:768], 256)
        left = z_buf[slot, at, 768:896]
        right = z_buf[slot, at, 896:1024]
        side = down(left, 128) + pltpu.roll(left, 64, 1) + up(right, 128)
        out = jnp.concatenate([main, side[:, 0:rem]], axis=1) + bias
        if index == 1:
            out = out + lat_buf[s, r].astype(F32)
        rounded = out.astype(BF16)
        if index == 0:
            y_out[s, r] = rounded
            back = rounded.astype(F32)
            acc[s][0] = acc[s][0] + fold_rows(back)
            acc[s][1] = acc[s][1] + fold_rows(back * back)
        else:
            kept = source_row(s, r)
            send_out[s, r] = jnp.where(sec == 0, rounded, kept)
            keep_out[s, r] = jnp.where(sec == 0, kept, rounded)

    row_a = jnp.where(even, rows - 1, 0)
    tasks = []
    for s in range(n):
        r0 = 0
        for count in chunks[s]:
            tasks.append((s, r0, count))
            r0 += count
    pending = None
    done = [0] * n

    def prepare(task):
        s, r0, count = task
        while done[s] < r0 + count + 2:
            normalize(s, done[s])
            done[s] += 1

    def complete(k):
        s, r0, count = tasks[k]
        for r in range(count):
            finish_row(s, r0 + r, k % 2, r)
        if index == 0 and r0 + count == rows:
            ha_out[s] = y_out[s, row_a]
            hb_out[s] = y_out[s, rows - 1 - row_a]

    early = EARLY[index]
    if index == 0:
        for k in range(early):
            prepare(tasks[k])
            multiply(*tasks[k], k % 2)
            if k > 0:
                complete(k - 1)
    else:
        for k in range(early):
            prepare(tasks[k])
    if index == 1:
        kernel_load.wait()
        lay_out(src, 0, w_ref)
    for cp in loads:
        cp.wait()
    for k, task in enumerate(tasks):
        if index == 0 and k < early:
            continue
        prepare(task)
        multiply(*task, k % 2)
        if k + 1 < len(tasks):
            prepare(tasks[k + 1])
        if k > 0:
            complete(k - 1)
    complete(len(tasks) - 1)
    if index == 0:
        rows_out = []
        for s in range(n):
            rows_out += [v.sum(axis=0, keepdims=True) for v in acc[s]]
        sums = jnp.concatenate(rows_out + [jnp.zeros((8 - 2 * n, ch), F32)], axis=0)
        send_group_sums(sums, stats_out, ch // GROUPS)


def keep_kernel(keep, full_out, sem):
    n = keep.shape[0]
    cp = pltpu.make_async_copy(keep, full_out.at[pl.ds(n * lax.axis_index("section"), n)], sem)
    cp.start()
    cp.wait()


def finish_kernel(full_in, received, full_out, sem):
    n = received.shape[0]
    at = jnp.where(lax.axis_index("section") == 0, n, 0)
    cp = pltpu.make_async_copy(received, full_out.at[pl.ds(at, n)], sem)
    cp.start()
    cp.wait()


def swap(array):
    return lax.ppermute(array, "section", [(0, 1), (1, 0)])


def on_device(latents, kernels, norm_gain, norm_bias, conv_bias):
    samples, rows, cols, ch = latents.shape
    n = samples // lax.axis_size("section")
    n_space = lax.axis_size("space")
    members = rows * n_space * cols * (ch // GROUPS)
    pairs_a = [(i, i ^ 1) for i in range(n_space)]
    pairs_b = [(i, (i - 1) % n_space if i % 2 == 0 else (i + 1) % n_space) for i in range(n_space)]
    shape = jax.ShapeDtypeStruct
    stats_shape = pltpu.VMEM((n_space, 8, 128), F32)
    edge_shape = pltpu.VMEM((n, cols, ch), BF16)
    part_shape = shape((n, rows, cols, ch), BF16)
    limit = pltpu.CompilerParams(vmem_limit_bytes=32 * 1024 * 1024)

    latents = pltpu.with_memory_space_constraint(latents, pltpu.HBM)
    kernels = pltpu.with_memory_space_constraint(kernels, pltpu.HBM)
    own_p = jnp.concatenate([norm_gain, norm_bias, conv_bias], axis=0)
    other_p = swap(own_p)
    other_k = pltpu.with_memory_space_constraint(swap(kernels), pltpu.HBM)

    stats, ha, hb = pl.pallas_call(
        stats_kernel,
        out_shape=(stats_shape, edge_shape, edge_shape),
        in_specs=[HBM],
        out_specs=(VM, VM, VM),
        scratch_shapes=[
            pltpu.VMEM((n, rows, cols, ch), BF16),
            pltpu.SemaphoreType.DMA((n,)),
        ],
        compiler_params=limit,
        name="stats",
    )(latents)
    ra = lax.ppermute(ha, "space", pairs_a)
    rb = lax.ppermute(hb, "space", pairs_b)
    stats = lax.all_to_all(stats, "space", split_axis=0, concat_axis=0, tiled=True)

    head = HEAD
    w_type = (1024, 1024)

    head_ref, w0 = pl.pallas_call(
        prepare_kernel,
        out_shape=(pltpu.VMEM((head, cols, ch), BF16), pltpu.VMEM(w_type, BF16)),
        in_specs=[HBM, HBM, HBM],
        out_specs=(VM, VM),
        scratch_shapes=[pltpu.VMEM(kernels.shape, BF16), pltpu.SemaphoreType.DMA((2,))],
        compiler_params=pltpu.CompilerParams(vmem_limit_bytes=16 * 1024 * 1024),
        name="prepare",
    )(kernels, other_k, latents)

    chunks = CHUNKS
    most = max(max(c) for c in chunks)

    def conv(index, operands, out_shape):
        body = lambda *refs: conv_kernel(index, members, n_space, chunks, *refs)
        return pl.pallas_call(
            body,
            out_shape=out_shape,
            in_specs=[VM] * 6 + [HBM, HBM, HBM] if index else [VM] * 7 + [HBM],
            out_specs=(VM,) * len(out_shape),
            scratch_shapes=[
                pltpu.VMEM((n, (rows + 2) * cols, 256), BF16),
                pltpu.VMEM((n, rows * cols, 256), BF16),
                pltpu.VMEM((n, rows + 2, cols, ch - 256), F32),
                pltpu.VMEM((2, most * cols, 1024), F32),
                pltpu.VMEM((n, rows, cols, ch), BF16),
                pltpu.SemaphoreType.DMA((n + 1,)),
                *([pltpu.VMEM(w_type, BF16), pltpu.VMEM(kernels.shape, BF16)] if index else []),
            ],
            compiler_params=limit,
            name="conv%d" % index,
        )(*operands)

    first, stats, ha, hb = conv(
        0,
        (ra, rb, stats, own_p, other_p, head_ref, w0, latents),
        (pltpu.VMEM(part_shape.shape, BF16), stats_shape, edge_shape, edge_shape),
    )
    ra = lax.ppermute(ha, "space", pairs_a)
    rb = lax.ppermute(hb, "space", pairs_b)
    stats = lax.all_to_all(stats, "space", split_axis=0, concat_axis=0, tiled=True)
    full_shape = shape((samples, rows, cols, ch), BF16)
    send, keep = conv(1, (ra, rb, stats, own_p, other_p, first, kernels, other_k, latents), (part_shape, part_shape))
    received = swap(send)
    small = pltpu.CompilerParams(vmem_limit_bytes=1024 * 1024)
    full = pl.pallas_call(
        keep_kernel,
        out_shape=full_shape,
        in_specs=[VM],
        out_specs=HBM,
        scratch_shapes=[pltpu.SemaphoreType.DMA],
        compiler_params=small,
        name="keep",
    )(keep)
    full = pl.pallas_call(
        finish_kernel,
        out_shape=full_shape,
        in_specs=[HBM, VM],
        out_specs=HBM,
        scratch_shapes=[pltpu.SemaphoreType.DMA],
        input_output_aliases={0: 0},
        compiler_params=small,
        name="finish",
    )(full, received)
    return full[None]


def solution(mesh):
    return jax.shard_map(
        on_device,
        mesh=mesh,
        in_specs=(
            P("dp", "space", None, None),
            P("section", None, None, None, None),
            P("section", None),
            P("section", None),
            P("section", None),
        ),
        out_specs=P("section", "dp", "space", None, None),
        check_vma=False,
    )
```

```python
import jax
import jax.numpy as jnp
from jax import lax
from jax.experimental import pallas as pl
from jax.experimental.pallas import tpu as pltpu
from jax.sharding import PartitionSpec as P

GROUPS = 32
HEAD = 5
EARLY = (2, 3, 1)
CHUNKS = ((2, 2, 2), (2, 2, 2))
F32 = jnp.float32
BF16 = jnp.bfloat16
ANY = pl.BlockSpec(memory_space=pl.ANY)
VM = pl.BlockSpec(memory_space=pltpu.VMEM)
HBM = pl.BlockSpec(memory_space=pltpu.HBM)


def one_hot(shape, channel_dim, per_group):
    channel = lax.broadcasted_iota(jnp.int32, shape, channel_dim)
    group = lax.broadcasted_iota(jnp.int32, shape, 1 - channel_dim)
    low = group * per_group
    return jnp.where((channel >= low) & (channel < low + per_group), 1.0, 0.0).astype(BF16)


def exact_dot(values, selector):
    high = values.astype(BF16)
    rest = values - high.astype(F32)
    middle = rest.astype(BF16)
    low = (rest - middle.astype(F32)).astype(BF16)
    return (
        jnp.dot(high, selector, preferred_element_type=F32)
        + jnp.dot(middle, selector, preferred_element_type=F32)
        + jnp.dot(low, selector, preferred_element_type=F32)
    )


def send_group_sums(sums, stats_out, per_group):
    channels = sums.shape[1]
    grouped = exact_dot(sums, one_hot((channels, 128), 0, per_group))
    for i in range(stats_out.shape[0]):
        stats_out[i] = grouped


def fold_rows(block):
    return block.reshape(block.shape[0] // 8, 8, block.shape[1]).sum(axis=0)


def stats_kernel(x_any, stats_out, ha_out, hb_out, x_buf, sem):
    n, rows, cols, ch = x_buf.shape
    sec = lax.axis_index("section")
    even = lax.axis_index("space") % 2 == 0
    loads = []
    for s in range(n):
        cp = pltpu.make_async_copy(x_any.at[sec * n + s], x_buf.at[s], sem.at[s])
        cp.start()
        loads.append(cp)
    total = []
    row_a = jnp.where(even, rows - 1, 0)
    for s in range(n):
        loads[s].wait()
        ha_out[s] = x_buf[s, row_a]
        hb_out[s] = x_buf[s, rows - 1 - row_a]

        def step(r, carry):
            acc, sq = carry
            v = x_buf[s, r].astype(F32)
            return acc + fold_rows(v), sq + fold_rows(v * v)

        zero = jnp.zeros((8, ch), F32)
        acc, sq = lax.fori_loop(0, rows, step, (zero, zero))
        total += [acc.sum(axis=0, keepdims=True), sq.sum(axis=0, keepdims=True)]
    sums = jnp.concatenate(total + [jnp.zeros((8 - len(total), ch), F32)], axis=0)
    send_group_sums(sums, stats_out, ch // GROUPS)


def lay_out(src, k, dst):
    ch = src.shape[-1]
    rem = ch - 256
    for dr in range(3):
        for dc in range(3):
            dst[dr * 256 : dr * 256 + 256, dc * 256 : dc * 256 + 256] = src[k, dr, dc, 0:256, 0:256]
            dst[768 + dr * rem : 768 + dr * rem + rem, dc * 256 : dc * 256 + 256] = src[k, dr, dc, 256:ch, 0:256]
        right = [src[k, dr, dc, :, 256:ch].astype(F32) for dc in range(3)]
        right = jnp.concatenate(right + [jnp.zeros((ch, 256 - 3 * rem), F32)], axis=1).astype(BF16)
        dst[dr * 256 : dr * 256 + 256, 768:1024] = right[0:256]
        dst[768 + dr * rem : 768 + dr * rem + rem, 768:1024] = right[256:ch]
    dst[768 + 3 * rem : 1024, :] = jnp.zeros((256 - 3 * rem, 1024), BF16)


def load_kernel(index, own_k, other_k, dst, sem):
    sec = lax.axis_index("section")

    @pl.when(sec == index)
    def _():
        pltpu.make_async_copy(own_k, dst, sem).start()

    @pl.when(sec != index)
    def _():
        pltpu.make_async_copy(other_k, dst, sem).start()

    return pltpu.make_async_copy(own_k, dst, sem)


def prepare_kernel(own_k, other_k, x_hbm, head_out, w_out, src, sem):
    head = head_out.shape[0]
    kernel_load = load_kernel(0, own_k, other_k, src, sem.at[0])
    at = lax.axis_index("section") * (x_hbm.shape[0] // 2)
    load = pltpu.make_async_copy(x_hbm.at[at, pl.ds(0, head)], head_out, sem.at[1])
    load.start()
    kernel_load.wait()
    lay_out(src, 0, w_out)
    load.wait()


def conv_kernel(index, which, members, n_space, chunks, *refs):
    if index == 0:
        (ra_ref, rb_ref, stats_ref, own_p, other_p, head_ref, w_ref, lat_hbm,
         y_out, stats_out, ha_out, hb_out,
         xm, xr, rem_buf, z_buf, lat_buf, sem) = refs
        head = head_ref.shape[0]
        loads = []
    elif which == 0:
        (ra_ref, rb_ref, stats_ref, own_p, other_p, x_ref, own_k, other_k, lat_hbm,
         send_out, keep_out, w_ref, lat_next,
         xm, xr, rem_buf, z_buf, lat_buf, sem, src) = refs
        head = 0
        kernel_load = load_kernel(1, own_k, other_k, src, sem.at[2])
        loads = []
    else:
        (ra_ref, rb_ref, stats_ref, own_p, other_p, x_ref, w_ref, lat_next,
         send_out, keep_out,
         xm, xr, rem_buf, z_buf) = refs
        loads = []
    n, rows, cols, ch = lat_buf.shape if index == 0 else x_ref.shape
    chosen = range(n) if index == 0 else (which,)
    padded_rows = rows + 2
    rem = ch - 256
    sec = lax.axis_index("section")
    space = lax.axis_index("space")
    even = space % 2 == 0
    if index == 0:
        for s in range(n):
            low = head if s == 0 else 0
            loads.append(
                pltpu.make_async_copy(
                    lat_hbm.at[sec * n + s, pl.ds(low, rows - low)], lat_buf.at[s, pl.ds(low, rows - low)], sem.at[s]
                )
            )
    elif which == 0:
        loads.append(pltpu.make_async_copy(lat_hbm.at[sec * n], lat_buf.at[0], sem.at[0]))
        next_load = pltpu.make_async_copy(lat_hbm.at[sec * n + 1], lat_next, sem.at[1])
    for cp in loads:
        cp.start()
    if index == 1 and which == 0:
        next_load.start()

    def source_row(s, r):
        if index == 1:
            return x_ref[s, r]
        if s == 0 and r < head:
            return head_ref[r]
        return lat_buf[s, r]

    params = jnp.where(sec == index, own_p[...], other_p[...])
    gain, shift, bias = params[0:1], params[1:2], params[2:3]
    total = stats_ref[0]
    for i in range(1, n_space):
        total = total + stats_ref[i]
    packed = []
    for s in range(n):
        mean = total[2 * s : 2 * s + 1] * (1.0 / members)
        var = jnp.maximum(total[2 * s + 1 : 2 * s + 2] * (1.0 / members) - mean * mean, 0.0)
        packed += [mean, lax.rsqrt(var + 1e-05)]
    packed = jnp.concatenate(packed + [jnp.zeros((8 - 2 * n, 128), F32)], axis=0)
    spread = exact_dot(packed, one_hot((128, ch), 1, ch // GROUPS))
    half_a = [0.5 * (spread[2 * s + 1 : 2 * s + 2] * gain) for s in range(n)]
    half_b = [0.5 * shift - spread[2 * s : 2 * s + 1] * half_a[s] for s in range(n)]

    def normalize(s, j):
        if j == 0:
            source = jnp.where(even, rb_ref[s], ra_ref[s])
        elif j == padded_rows - 1:
            source = jnp.where(even, ra_ref[s], rb_ref[s])
        else:
            source = source_row(s, j - 1)
        half = source.astype(F32) * half_a[s] + half_b[s]
        y = half + half * jnp.tanh(half)
        if j == 0:
            y = jnp.where(space == 0, 0.0, y)
        if j == padded_rows - 1:
            y = jnp.where(space == n_space - 1, 0.0, y)
        xm[s, pl.ds(j * cols, cols), :] = y[:, 0:256].astype(BF16)
        rem_buf[s, j] = y[:, 256:ch]
        if j >= 2:
            parts = [rem_buf[s, j - 2], rem_buf[s, j - 1], rem_buf[s, j], jnp.zeros((cols, 256 - 3 * rem), F32)]
            xr[s, pl.ds((j - 2) * cols, cols), :] = jnp.concatenate(parts, axis=1).astype(BF16)

    def multiply(s, r0, count, slot):
        m = count * cols
        lhs = jnp.concatenate(
            [xm[s, pl.ds((r0 + dr) * cols, m), :] for dr in range(3)] + [xr[s, pl.ds(r0 * cols, m), :]],
            axis=1,
        )
        z_buf[slot, 0:m, :] = jnp.dot(lhs, w_ref[...], preferred_element_type=F32)

    first_slab = lax.broadcasted_iota(jnp.int32, (8, 256), 0) == 0
    last_slab = lax.broadcasted_iota(jnp.int32, (8, 256), 0) == 7

    def down(z, width):
        moved = pltpu.roll(z, 1, 0)
        head = jnp.where(first_slab[:, :width], 0.0, moved[0:8])
        return jnp.concatenate([head, moved[8:]], axis=0)

    def up(z, width):
        moved = pltpu.roll(z, cols - 1, 0)
        tail = jnp.where(last_slab[:, :width], 0.0, moved[cols - 8 :])
        return jnp.concatenate([moved[: cols - 8], tail], axis=0)

    acc = [[jnp.zeros((8, ch), F32) for _ in range(2)] for _ in range(n)]

    def finish_row(s, r, slot, at):
        at = pl.ds(at * cols, cols)
        main = z_buf[slot, at, 256:512] + down(z_buf[slot, at, 0:256], 256) + up(z_buf[slot, at, 512:768], 256)
        left = z_buf[slot, at, 768:896]
        right = z_buf[slot, at, 896:1024]
        side = down(left, 128) + pltpu.roll(left, 64, 1) + up(right, 128)
        out = jnp.concatenate([main, side[:, 0:rem]], axis=1) + bias
        if index == 1:
            out = out + (lat_buf[0, r] if which == 0 else lat_next[r]).astype(F32)
        rounded = out.astype(BF16)
        if index == 0:
            y_out[s, r] = rounded
            back = rounded.astype(F32)
            acc[s][0] = acc[s][0] + fold_rows(back)
            acc[s][1] = acc[s][1] + fold_rows(back * back)
        else:
            kept = source_row(s, r)
            send_out[r] = jnp.where(sec == 0, rounded, kept)
            keep_out[r] = jnp.where(sec == 0, kept, rounded)

    row_a = jnp.where(even, rows - 1, 0)
    tasks = []
    for s in chosen:
        r0 = 0
        for count in chunks[s]:
            tasks.append((s, r0, count))
            r0 += count
    pending = None
    done = [0] * n

    def prepare(task):
        s, r0, count = task
        while done[s] < r0 + count + 2:
            normalize(s, done[s])
            done[s] += 1

    def complete(k):
        s, r0, count = tasks[k]
        for r in range(count):
            finish_row(s, r0 + r, k % 2, r)
        if index == 0 and r0 + count == rows:
            ha_out[s] = y_out[s, row_a]
            hb_out[s] = y_out[s, rows - 1 - row_a]

    early = EARLY[index + which]
    if index == 0:
        for k in range(early):
            prepare(tasks[k])
            multiply(*tasks[k], k % 2)
            if k > 0:
                complete(k - 1)
    else:
        for k in range(early):
            prepare(tasks[k])
    if index == 1 and which == 0:
        kernel_load.wait()
        lay_out(src, 0, w_ref)
    for cp in loads:
        cp.wait()
    for k, task in enumerate(tasks):
        if index == 0 and k < early:
            continue
        prepare(task)
        multiply(*task, k % 2)
        if k + 1 < len(tasks):
            prepare(tasks[k + 1])
        if k > 0:
            complete(k - 1)
    complete(len(tasks) - 1)
    if index == 1 and which == 0:
        next_load.wait()
    if index == 0:
        rows_out = []
        for s in range(n):
            rows_out += [v.sum(axis=0, keepdims=True) for v in acc[s]]
        sums = jnp.concatenate(rows_out + [jnp.zeros((8 - 2 * n, ch), F32)], axis=0)
        send_group_sums(sums, stats_out, ch // GROUPS)


def keep_kernel(keep_0, keep_1, received, full_out, sem):
    sec = lax.axis_index("section")
    copies = [
        pltpu.make_async_copy(keep_0, full_out.at[2 * sec], sem.at[0]),
        pltpu.make_async_copy(keep_1, full_out.at[2 * sec + 1], sem.at[1]),
        pltpu.make_async_copy(received, full_out.at[2 - 2 * sec], sem.at[2]),
    ]
    for cp in copies:
        cp.start()
    for cp in copies:
        cp.wait()


def finish_kernel(full_in, received, full_out, sem):
    cp = pltpu.make_async_copy(received, full_out.at[3 - 2 * lax.axis_index("section")], sem)
    cp.start()
    cp.wait()


def swap(array):
    return lax.ppermute(array, "section", [(0, 1), (1, 0)])


def on_device(latents, kernels, norm_gain, norm_bias, conv_bias):
    samples, rows, cols, ch = latents.shape
    n = samples // lax.axis_size("section")
    n_space = lax.axis_size("space")
    members = rows * n_space * cols * (ch // GROUPS)
    pairs_a = [(i, i ^ 1) for i in range(n_space)]
    pairs_b = [(i, (i - 1) % n_space if i % 2 == 0 else (i + 1) % n_space) for i in range(n_space)]
    shape = jax.ShapeDtypeStruct
    stats_shape = pltpu.VMEM((n_space, 8, 128), F32)
    edge_shape = pltpu.VMEM((n, cols, ch), BF16)
    part_shape = shape((n, rows, cols, ch), BF16)
    limit = pltpu.CompilerParams(vmem_limit_bytes=32 * 1024 * 1024)

    latents = pltpu.with_memory_space_constraint(latents, pltpu.HBM)
    kernels = pltpu.with_memory_space_constraint(kernels, pltpu.HBM)
    own_p = jnp.concatenate([norm_gain, norm_bias, conv_bias], axis=0)
    other_p = swap(own_p)
    other_k = pltpu.with_memory_space_constraint(swap(kernels), pltpu.HBM)

    stats, ha, hb = pl.pallas_call(
        stats_kernel,
        out_shape=(stats_shape, edge_shape, edge_shape),
        in_specs=[HBM],
        out_specs=(VM, VM, VM),
        scratch_shapes=[
            pltpu.VMEM((n, rows, cols, ch), BF16),
            pltpu.SemaphoreType.DMA((n,)),
        ],
        compiler_params=limit,
        name="stats",
    )(latents)
    ra = lax.ppermute(ha, "space", pairs_a)
    rb = lax.ppermute(hb, "space", pairs_b)
    stats = lax.all_to_all(stats, "space", split_axis=0, concat_axis=0, tiled=True)

    head = HEAD
    w_type = (1024, 1024)

    head_ref, w0 = pl.pallas_call(
        prepare_kernel,
        out_shape=(pltpu.VMEM((head, cols, ch), BF16), pltpu.VMEM(w_type, BF16)),
        in_specs=[HBM, HBM, HBM],
        out_specs=(VM, VM),
        scratch_shapes=[pltpu.VMEM(kernels.shape, BF16), pltpu.SemaphoreType.DMA((2,))],
        compiler_params=pltpu.CompilerParams(vmem_limit_bytes=16 * 1024 * 1024),
        name="prepare",
    )(kernels, other_k, latents)

    chunks = CHUNKS
    most = max(max(c) for c in chunks)

    def conv(index, which, operands, out_shape):
        body = lambda *refs: conv_kernel(index, which, members, n_space, chunks, *refs)
        in_hbm = (1, 3, 0)[index + which]
        if index == 0:
            extra = [pltpu.VMEM((n, rows, cols, ch), BF16), pltpu.SemaphoreType.DMA((n,))]
        elif which == 0:
            extra = [
                pltpu.VMEM((1, rows, cols, ch), BF16),
                pltpu.SemaphoreType.DMA((3,)),
                pltpu.VMEM(kernels.shape, BF16),
            ]
        else:
            extra = []
        return pl.pallas_call(
            body,
            out_shape=out_shape,
            in_specs=[VM] * (len(operands) - in_hbm) + [HBM] * in_hbm,
            out_specs=(VM,) * len(out_shape),
            scratch_shapes=[
                pltpu.VMEM((n, (rows + 2) * cols, 256), BF16),
                pltpu.VMEM((n, rows * cols, 256), BF16),
                pltpu.VMEM((n, rows + 2, cols, ch - 256), F32),
                pltpu.VMEM((2, most * cols, 1024), F32),
                *extra,
            ],
            compiler_params=limit,
            name="conv%d%d" % (index, which),
        )(*operands)

    first, stats, ha, hb = conv(
        0,
        0,
        (ra, rb, stats, own_p, other_p, head_ref, w0, latents),
        (pltpu.VMEM(part_shape.shape, BF16), stats_shape, edge_shape, edge_shape),
    )
    ra = lax.ppermute(ha, "space", pairs_a)
    rb = lax.ppermute(hb, "space", pairs_b)
    stats = lax.all_to_all(stats, "space", split_axis=0, concat_axis=0, tiled=True)
    full_shape = shape((samples, rows, cols, ch), BF16)
    common = (ra, rb, stats, own_p, other_p, first)
    sample_shape = pltpu.VMEM((rows, cols, ch), BF16)
    send_0, keep_0, w1, lat_next = conv(
        1, 0, (*common, kernels, other_k, latents), (sample_shape, sample_shape, pltpu.VMEM(w_type, BF16), sample_shape)
    )
    received_0 = swap(send_0)
    send_1, keep_1 = conv(1, 1, (*common, w1, lat_next), (sample_shape, sample_shape))
    received_1 = swap(send_1)
    small = pltpu.CompilerParams(vmem_limit_bytes=1024 * 1024)
    full = pl.pallas_call(
        keep_kernel,
        out_shape=full_shape,
        in_specs=[VM, VM, VM],
        out_specs=HBM,
        scratch_shapes=[pltpu.SemaphoreType.DMA((3,))],
        compiler_params=small,
        name="keep",
    )(keep_0, keep_1, received_0)
    full = pl.pallas_call(
        finish_kernel,
        out_shape=full_shape,
        in_specs=[HBM, VM],
        out_specs=HBM,
        scratch_shapes=[pltpu.SemaphoreType.DMA],
        input_output_aliases={0: 0},
        compiler_params=small,
        name="finish",
    )(full, received_1)
    return full[None]


def solution(mesh):
    return jax.shard_map(
        on_device,
        mesh=mesh,
        in_specs=(
            P("dp", "space", None, None),
            P("section", None, None, None, None),
            P("section", None),
            P("section", None),
            P("section", None),
        ),
        out_specs=P("section", "dp", "space", None, None),
        check_vma=False,
    )
```

```python
import jax
import jax.numpy as jnp
from jax import lax
from jax.experimental import pallas as pl
from jax.experimental.pallas import tpu as pltpu
from jax.sharding import PartitionSpec as P

GROUPS = 32
HEAD = 5
EARLY = (2, 3, 1)
CHUNKS = ((2, 2, 2), (3, 3))
F32 = jnp.float32
BF16 = jnp.bfloat16
ANY = pl.BlockSpec(memory_space=pl.ANY)
VM = pl.BlockSpec(memory_space=pltpu.VMEM)
HBM = pl.BlockSpec(memory_space=pltpu.HBM)


def one_hot(shape, channel_dim, per_group):
    channel = lax.broadcasted_iota(jnp.int32, shape, channel_dim)
    group = lax.broadcasted_iota(jnp.int32, shape, 1 - channel_dim)
    low = group * per_group
    return jnp.where((channel >= low) & (channel < low + per_group), 1.0, 0.0).astype(BF16)


def exact_dot(values, selector):
    high = values.astype(BF16)
    rest = values - high.astype(F32)
    middle = rest.astype(BF16)
    low = (rest - middle.astype(F32)).astype(BF16)
    return (
        jnp.dot(high, selector, preferred_element_type=F32)
        + jnp.dot(middle, selector, preferred_element_type=F32)
        + jnp.dot(low, selector, preferred_element_type=F32)
    )


def send_group_sums(sums, stats_out, per_group):
    channels = sums.shape[1]
    grouped = exact_dot(sums, one_hot((channels, 128), 0, per_group))
    for i in range(stats_out.shape[0]):
        stats_out[i] = grouped


def fold_rows(block):
    return block.reshape(block.shape[0] // 8, 8, block.shape[1]).sum(axis=0)


def stats_kernel(x_any, stats_out, ha_out, hb_out, x_buf, sem):
    n, rows, cols, ch = x_buf.shape
    sec = lax.axis_index("section")
    even = lax.axis_index("space") % 2 == 0
    loads = []
    for s in range(n):
        cp = pltpu.make_async_copy(x_any.at[sec * n + s], x_buf.at[s], sem.at[s])
        cp.start()
        loads.append(cp)
    total = []
    row_a = jnp.where(even, rows - 1, 0)
    for s in range(n):
        loads[s].wait()
        ha_out[s] = x_buf[s, row_a]
        hb_out[s] = x_buf[s, rows - 1 - row_a]

        def step(r, carry):
            acc, sq = carry
            v = x_buf[s, r].astype(F32)
            return acc + fold_rows(v), sq + fold_rows(v * v)

        zero = jnp.zeros((8, ch), F32)
        acc, sq = lax.fori_loop(0, rows, step, (zero, zero))
        total += [acc.sum(axis=0, keepdims=True), sq.sum(axis=0, keepdims=True)]
    sums = jnp.concatenate(total + [jnp.zeros((8 - len(total), ch), F32)], axis=0)
    send_group_sums(sums, stats_out, ch // GROUPS)


def lay_out(src, k, dst):
    ch = src.shape[-1]
    rem = ch - 256
    for dr in range(3):
        for dc in range(3):
            dst[dr * 256 : dr * 256 + 256, dc * 256 : dc * 256 + 256] = src[k, dr, dc, 0:256, 0:256]
            dst[768 + dr * rem : 768 + dr * rem + rem, dc * 256 : dc * 256 + 256] = src[k, dr, dc, 256:ch, 0:256]
        right = [src[k, dr, dc, :, 256:ch].astype(F32) for dc in range(3)]
        right = jnp.concatenate(right + [jnp.zeros((ch, 256 - 3 * rem), F32)], axis=1).astype(BF16)
        dst[dr * 256 : dr * 256 + 256, 768:1024] = right[0:256]
        dst[768 + dr * rem : 768 + dr * rem + rem, 768:1024] = right[256:ch]
    dst[768 + 3 * rem : 1024, :] = jnp.zeros((256 - 3 * rem, 1024), BF16)


def prepare_kernel(x_hbm, own_k, other_k, head_out, w0_out, w1_hbm, src, w1_buf, sem):
    head = head_out.shape[0]
    sec = lax.axis_index("section")

    @pl.when(sec == 0)
    def _():
        pltpu.make_async_copy(other_k.at[0], src.at[1], sem.at[1]).start()
        pltpu.make_async_copy(own_k.at[0], src.at[0], sem.at[0]).start()

    @pl.when(sec != 0)
    def _():
        pltpu.make_async_copy(own_k.at[0], src.at[1], sem.at[1]).start()
        pltpu.make_async_copy(other_k.at[0], src.at[0], sem.at[0]).start()

    load = pltpu.make_async_copy(x_hbm.at[sec * (x_hbm.shape[0] // 2), pl.ds(0, head)], head_out, sem.at[2])
    load.start()
    pltpu.make_async_copy(own_k.at[0], src.at[1], sem.at[1]).wait()
    lay_out(src, 1, w1_buf)
    store = pltpu.make_async_copy(w1_buf, w1_hbm, sem.at[3])
    store.start()
    pltpu.make_async_copy(own_k.at[0], src.at[0], sem.at[0]).wait()
    lay_out(src, 0, w0_out)
    load.wait()
    store.wait()


def conv_kernel(index, which, members, n_space, chunks, *refs):
    if index == 0:
        (ra_ref, rb_ref, stats_ref, own_p, other_p, head_ref, w_ref, lat_hbm,
         y_out, stats_out, ha_out, hb_out,
         xm, xr, rem_buf, z_buf, lat_buf, sem) = refs
        head = head_ref.shape[0]
        loads = []
        planes = [(xm.at[s], xr.at[s]) for s in range(2)]
    elif which == 0:
        (ra_ref, rb_ref, stats_ref, own_p, other_p, x_ref, w_hbm, lat_hbm,
         send_out, keep_out, w_ref, lat_next, xm_next, xr_next,
         xm, xr, rem_buf, z_buf, lat_buf, sem) = refs
        head = 0
        loads = [pltpu.make_async_copy(w_hbm, w_ref, sem.at[2])]
        planes = [(xm.at[0], xr.at[0]), (xm_next, xr_next)]
    else:
        (own_p, other_p, x_ref, w_ref, lat_next, xm_next, xr_next,
         send_out, keep_out,
         z_buf) = refs
        loads = []
        planes = [None, (xm_next, xr_next)]
    n, rows, cols, ch = lat_buf.shape if index == 0 else x_ref.shape
    chosen = range(n) if index == 0 else (which,)
    padded_rows = rows + 2
    rem = ch - 256
    sec = lax.axis_index("section")
    space = lax.axis_index("space")
    even = space % 2 == 0
    if index == 0:
        for s in range(n):
            low = head if s == 0 else 0
            loads.append(
                pltpu.make_async_copy(
                    lat_hbm.at[sec * n + s, pl.ds(low, rows - low)], lat_buf.at[s, pl.ds(low, rows - low)], sem.at[s]
                )
            )
    elif which == 0:
        loads.append(pltpu.make_async_copy(lat_hbm.at[sec * n], lat_buf.at[0], sem.at[0]))
        next_load = pltpu.make_async_copy(lat_hbm.at[sec * n + 1], lat_next, sem.at[1])
    for cp in loads:
        cp.start()
    if index == 1 and which == 0:
        next_load.start()

    def source_row(s, r):
        if index == 1:
            return x_ref[s, r]
        if s == 0 and r < head:
            return head_ref[r]
        return lat_buf[s, r]

    params = jnp.where(sec == index, own_p[...], other_p[...])
    gain, shift, bias = params[0:1], params[1:2], params[2:3]
    if index + which < 2:
        total = stats_ref[0]
        for i in range(1, n_space):
            total = total + stats_ref[i]
        packed = []
        for s in range(n):
            mean = total[2 * s : 2 * s + 1] * (1.0 / members)
            var = jnp.maximum(total[2 * s + 1 : 2 * s + 2] * (1.0 / members) - mean * mean, 0.0)
            packed += [mean, lax.rsqrt(var + 1e-05)]
        packed = jnp.concatenate(packed + [jnp.zeros((8 - 2 * n, 128), F32)], axis=0)
        spread = exact_dot(packed, one_hot((128, ch), 1, ch // GROUPS))
        half_a = [0.5 * (spread[2 * s + 1 : 2 * s + 2] * gain) for s in range(n)]
        half_b = [0.5 * shift - spread[2 * s : 2 * s + 1] * half_a[s] for s in range(n)]

    def normalize(s, j):
        if j == 0:
            source = jnp.where(even, rb_ref[s], ra_ref[s])
        elif j == padded_rows - 1:
            source = jnp.where(even, ra_ref[s], rb_ref[s])
        else:
            source = source_row(s, j - 1)
        half = source.astype(F32) * half_a[s] + half_b[s]
        y = half + half * jnp.tanh(half)
        if j == 0:
            y = jnp.where(space == 0, 0.0, y)
        if j == padded_rows - 1:
            y = jnp.where(space == n_space - 1, 0.0, y)
        planes[s][0][pl.ds(j * cols, cols), :] = y[:, 0:256].astype(BF16)
        rem_buf[s, j] = y[:, 256:ch]
        if j >= 2:
            parts = [rem_buf[s, j - 2], rem_buf[s, j - 1], rem_buf[s, j], jnp.zeros((cols, 256 - 3 * rem), F32)]
            planes[s][1][pl.ds((j - 2) * cols, cols), :] = jnp.concatenate(parts, axis=1).astype(BF16)

    def multiply(s, r0, count, slot):
        m = count * cols
        lhs = jnp.concatenate(
            [planes[s][0][pl.ds((r0 + dr) * cols, m), :] for dr in range(3)] + [planes[s][1][pl.ds(r0 * cols, m), :]],
            axis=1,
        )
        z_buf[slot, 0:m, :] = jnp.dot(lhs, w_ref[...], preferred_element_type=F32)

    first_slab = lax.broadcasted_iota(jnp.int32, (8, 256), 0) == 0
    last_slab = lax.broadcasted_iota(jnp.int32, (8, 256), 0) == 7

    def down(z, width):
        moved = pltpu.roll(z, 1, 0)
        head = jnp.where(first_slab[:, :width], 0.0, moved[0:8])
        return jnp.concatenate([head, moved[8:]], axis=0)

    def up(z, width):
        moved = pltpu.roll(z, cols - 1, 0)
        tail = jnp.where(last_slab[:, :width], 0.0, moved[cols - 8 :])
        return jnp.concatenate([moved[: cols - 8], tail], axis=0)

    acc = [[jnp.zeros((8, ch), F32) for _ in range(2)] for _ in range(n)]

    def finish_row(s, r, slot, at):
        at = pl.ds(at * cols, cols)
        main = z_buf[slot, at, 256:512] + down(z_buf[slot, at, 0:256], 256) + up(z_buf[slot, at, 512:768], 256)
        left = z_buf[slot, at, 768:896]
        right = z_buf[slot, at, 896:1024]
        side = down(left, 128) + pltpu.roll(left, 64, 1) + up(right, 128)
        out = jnp.concatenate([main, side[:, 0:rem]], axis=1) + bias
        if index == 1:
            out = out + (lat_buf[0, r] if which == 0 else lat_next[r]).astype(F32)
        rounded = out.astype(BF16)
        if index == 0:
            y_out[s, r] = rounded
            back = rounded.astype(F32)
            acc[s][0] = acc[s][0] + fold_rows(back)
            acc[s][1] = acc[s][1] + fold_rows(back * back)
        else:
            kept = source_row(s, r)
            send_out[r] = jnp.where(sec == 0, rounded, kept)
            keep_out[r] = jnp.where(sec == 0, kept, rounded)

    row_a = jnp.where(even, rows - 1, 0)
    tasks = []
    for s in chosen:
        r0 = 0
        for count in chunks[s]:
            tasks.append((s, r0, count))
            r0 += count
    pending = None
    done = [0] * n

    def prepare(task):
        s, r0, count = task
        if index + which == 2:
            return
        while done[s] < r0 + count + 2:
            normalize(s, done[s])
            done[s] += 1

    def complete(k):
        s, r0, count = tasks[k]
        for r in range(count):
            finish_row(s, r0 + r, k % 2, r)
        if index == 0 and r0 + count == rows:
            ha_out[s] = y_out[s, row_a]
            hb_out[s] = y_out[s, rows - 1 - row_a]

    early = EARLY[index + which]
    if index == 0:
        for k in range(early):
            prepare(tasks[k])
            multiply(*tasks[k], k % 2)
            if k > 0:
                complete(k - 1)
    else:
        for s in range(n) if which == 0 else ():
            for j in range(padded_rows):
                normalize(s, j)
            done[s] = padded_rows
    for cp in loads:
        cp.wait()
    for k, task in enumerate(tasks):
        if index == 0 and k < early:
            continue
        prepare(task)
        multiply(*task, k % 2)
        if k + 1 < len(tasks):
            prepare(tasks[k + 1])
        if k > 0:
            complete(k - 1)
    complete(len(tasks) - 1)
    if index == 1 and which == 0:
        next_load.wait()
    if index == 0:
        rows_out = []
        for s in range(n):
            rows_out += [v.sum(axis=0, keepdims=True) for v in acc[s]]
        sums = jnp.concatenate(rows_out + [jnp.zeros((8 - 2 * n, ch), F32)], axis=0)
        send_group_sums(sums, stats_out, ch // GROUPS)


def keep_kernel(keep_0, keep_1, received, full_out, sem):
    sec = lax.axis_index("section")
    copies = [
        pltpu.make_async_copy(keep_0, full_out.at[2 * sec], sem.at[0]),
        pltpu.make_async_copy(keep_1, full_out.at[2 * sec + 1], sem.at[1]),
        pltpu.make_async_copy(received, full_out.at[2 - 2 * sec], sem.at[2]),
    ]
    for cp in copies:
        cp.start()
    for cp in copies:
        cp.wait()


def finish_kernel(full_in, received, full_out, sem):
    cp = pltpu.make_async_copy(received, full_out.at[3 - 2 * lax.axis_index("section")], sem)
    cp.start()
    cp.wait()


def swap(array):
    return lax.ppermute(array, "section", [(0, 1), (1, 0)])


def on_device(latents, kernels, norm_gain, norm_bias, conv_bias):
    samples, rows, cols, ch = latents.shape
    n = samples // lax.axis_size("section")
    n_space = lax.axis_size("space")
    members = rows * n_space * cols * (ch // GROUPS)
    pairs_a = [(i, i ^ 1) for i in range(n_space)]
    pairs_b = []
    for c in range(lax.axis_size("section")):
        pairs_b += [(c * n_space + e, (1 - c) * n_space + e) for e in (0, n_space - 1)]
        pairs_b += [(c * n_space + i, c * n_space + (i - 1 if i % 2 == 0 else i + 1)) for i in range(1, n_space - 1)]
    shape = jax.ShapeDtypeStruct
    stats_shape = pltpu.VMEM((n_space, 8, 128), F32)
    edge_shape = pltpu.VMEM((n, cols, ch), BF16)
    part_shape = shape((n, rows, cols, ch), BF16)
    limit = pltpu.CompilerParams(vmem_limit_bytes=32 * 1024 * 1024)

    latents = pltpu.with_memory_space_constraint(latents, pltpu.HBM)
    kernels = pltpu.with_memory_space_constraint(kernels, pltpu.HBM)
    own_p = jnp.concatenate([norm_gain, norm_bias, conv_bias], axis=0)
    other_p = swap(own_p)
    other_k = pltpu.with_memory_space_constraint(swap(kernels), pltpu.HBM)

    stats, ha, hb = pl.pallas_call(
        stats_kernel,
        out_shape=(stats_shape, edge_shape, edge_shape),
        in_specs=[HBM],
        out_specs=(VM, VM, VM),
        scratch_shapes=[
            pltpu.VMEM((n, rows, cols, ch), BF16),
            pltpu.SemaphoreType.DMA((n,)),
        ],
        compiler_params=limit,
        name="stats",
    )(latents)
    ra = lax.ppermute(ha, "space", pairs_a)
    rb = lax.ppermute(hb, ("section", "space"), pairs_b)
    stats = lax.all_to_all(stats, "space", split_axis=0, concat_axis=0, tiled=True)

    head = HEAD
    w_type = (1024, 1024)

    head_ref, w0, w1 = pl.pallas_call(
        prepare_kernel,
        out_shape=(pltpu.VMEM((head, cols, ch), BF16), pltpu.VMEM(w_type, BF16), pltpu.HBM(w_type, BF16)),
        in_specs=[HBM, HBM, HBM],
        out_specs=(VM, VM, HBM),
        scratch_shapes=[
            pltpu.VMEM((2, *kernels.shape[1:]), BF16),
            pltpu.VMEM(w_type, BF16),
            pltpu.SemaphoreType.DMA((4,)),
        ],
        compiler_params=pltpu.CompilerParams(vmem_limit_bytes=16 * 1024 * 1024),
        name="prepare",
    )(latents, kernels, other_k)
    w1 = pltpu.with_memory_space_constraint(w1, pltpu.HBM)

    chunks = CHUNKS
    most = max(max(c) for c in chunks)

    def conv(index, which, operands, out_shape):
        body = lambda *refs: conv_kernel(index, which, members, n_space, chunks, *refs)
        in_hbm = (1, 2, 0)[index + which]
        z_type = pltpu.VMEM((2, most * cols, 1024), F32)
        if index + which < 2:
            held = n if index == 0 else 1
            scratch = [
                pltpu.VMEM((held, (rows + 2) * cols, 256), BF16),
                pltpu.VMEM((held, rows * cols, 256), BF16),
                pltpu.VMEM((n, rows + 2, cols, ch - 256), F32),
                z_type,
                pltpu.VMEM((held, rows, cols, ch), BF16),
                pltpu.SemaphoreType.DMA((3,)),
            ]
        else:
            scratch = [z_type]
        return pl.pallas_call(
            body,
            out_shape=out_shape,
            in_specs=[VM] * (len(operands) - in_hbm) + [HBM] * in_hbm,
            out_specs=(VM,) * len(out_shape),
            scratch_shapes=scratch,
            compiler_params=limit,
            name="conv%d%d" % (index, which),
        )(*operands)

    first, stats, ha, hb = conv(
        0,
        0,
        (ra, rb, stats, own_p, other_p, head_ref, w0, latents),
        (pltpu.VMEM(part_shape.shape, BF16), stats_shape, edge_shape, edge_shape),
    )
    ra = lax.ppermute(ha, "space", pairs_a)
    rb = lax.ppermute(hb, ("section", "space"), pairs_b)
    stats = lax.all_to_all(stats, "space", split_axis=0, concat_axis=0, tiled=True)
    full_shape = shape((samples, rows, cols, ch), BF16)
    common = (ra, rb, stats, own_p, other_p, first)
    sample_shape = pltpu.VMEM((rows, cols, ch), BF16)
    plane_shapes = (pltpu.VMEM(((rows + 2) * cols, 256), BF16), pltpu.VMEM((rows * cols, 256), BF16))
    send_0, keep_0, *rest = conv(
        1,
        0,
        (*common, w1, latents),
        (sample_shape, sample_shape, pltpu.VMEM(w_type, BF16), sample_shape, *plane_shapes),
    )
    received_0 = swap(send_0)
    send_1, keep_1 = conv(1, 1, (own_p, other_p, first, *rest), (sample_shape, sample_shape))
    received_1 = swap(send_1)
    small = pltpu.CompilerParams(vmem_limit_bytes=1024 * 1024)
    full = pl.pallas_call(
        keep_kernel,
        out_shape=full_shape,
        in_specs=[VM, VM, VM],
        out_specs=HBM,
        scratch_shapes=[pltpu.SemaphoreType.DMA((3,))],
        compiler_params=small,
        name="keep",
    )(keep_0, keep_1, received_0)
    full = pl.pallas_call(
        finish_kernel,
        out_shape=full_shape,
        in_specs=[HBM, VM],
        out_specs=HBM,
        scratch_shapes=[pltpu.SemaphoreType.DMA],
        input_output_aliases={0: 0},
        compiler_params=small,
        name="finish",
    )(full, received_1)
    return full[None]


def solution(mesh):
    return jax.shard_map(
        on_device,
        mesh=mesh,
        in_specs=(
            P("dp", "space", None, None),
            P("section", None, None, None, None),
            P("section", None),
            P("section", None),
            P("section", None),
        ),
        out_specs=P("section", "dp", "space", None, None),
        check_vma=False,
    )
```

```python
import jax
import jax.numpy as jnp
from jax import lax
from jax.experimental import pallas as pl
from jax.experimental.pallas import tpu as pltpu
from jax.sharding import PartitionSpec as P

GROUPS = 32
MORE = 2
HEAD = 5
EARLY = (2, 3, 1)
CHUNKS = ((2, 2, 2), (2, 2, 2))
F32 = jnp.float32
BF16 = jnp.bfloat16
ANY = pl.BlockSpec(memory_space=pl.ANY)
VM = pl.BlockSpec(memory_space=pltpu.VMEM)
HBM = pl.BlockSpec(memory_space=pltpu.HBM)


def one_hot(shape, channel_dim, per_group):
    channel = lax.broadcasted_iota(jnp.int32, shape, channel_dim)
    group = lax.broadcasted_iota(jnp.int32, shape, 1 - channel_dim)
    low = group * per_group
    return jnp.where((channel >= low) & (channel < low + per_group), 1.0, 0.0).astype(BF16)


def exact_dot(values, selector):
    high = values.astype(BF16)
    rest = values - high.astype(F32)
    middle = rest.astype(BF16)
    low = (rest - middle.astype(F32)).astype(BF16)
    return (
        jnp.dot(high, selector, preferred_element_type=F32)
        + jnp.dot(middle, selector, preferred_element_type=F32)
        + jnp.dot(low, selector, preferred_element_type=F32)
    )


def send_group_sums(sums, stats_out, per_group):
    channels = sums.shape[1]
    grouped = exact_dot(sums, one_hot((channels, 128), 0, per_group))
    for i in range(stats_out.shape[0]):
        stats_out[i] = grouped


def fold_rows(block):
    return block.reshape(block.shape[0] // 8, 8, block.shape[1]).sum(axis=0)


def stats_kernel(x_any, stats_out, ha_out, hb_out, x_buf, sem):
    n, rows, cols, ch = x_buf.shape
    sec = lax.axis_index("section")
    even = lax.axis_index("space") % 2 == 0
    loads = []
    for s in range(n):
        cp = pltpu.make_async_copy(x_any.at[sec * n + s], x_buf.at[s], sem.at[s])
        cp.start()
        loads.append(cp)
    total = []
    row_a = jnp.where(even, rows - 1, 0)
    for s in range(n):
        loads[s].wait()
        ha_out[s] = x_buf[s, row_a]
        hb_out[s] = x_buf[s, rows - 1 - row_a]

        def step(r, carry):
            acc, sq = carry
            v = x_buf[s, r].astype(F32)
            return acc + fold_rows(v), sq + fold_rows(v * v)

        zero = jnp.zeros((8, ch), F32)
        acc, sq = lax.fori_loop(0, rows, step, (zero, zero))
        total += [acc.sum(axis=0, keepdims=True), sq.sum(axis=0, keepdims=True)]
    sums = jnp.concatenate(total + [jnp.zeros((8 - len(total), ch), F32)], axis=0)
    send_group_sums(sums, stats_out, ch // GROUPS)


def lay_out(src, k, dst):
    ch = src.shape[-1]
    rem = ch - 256
    for dr in range(3):
        for dc in range(3):
            dst[dr * 256 : dr * 256 + 256, dc * 256 : dc * 256 + 256] = src[k, dr, dc, 0:256, 0:256]
            dst[768 + dr * rem : 768 + dr * rem + rem, dc * 256 : dc * 256 + 256] = src[k, dr, dc, 256:ch, 0:256]
        right = [src[k, dr, dc, :, 256:ch].astype(F32) for dc in range(3)]
        right = jnp.concatenate(right + [jnp.zeros((ch, 256 - 3 * rem), F32)], axis=1).astype(BF16)
        dst[dr * 256 : dr * 256 + 256, 768:1024] = right[0:256]
        dst[768 + dr * rem : 768 + dr * rem + rem, 768:1024] = right[256:ch]
    dst[768 + 3 * rem : 1024, :] = jnp.zeros((256 - 3 * rem, 1024), BF16)


def prepare_kernel(x_hbm, own_k, other_k, head_out, w0_out, w1_hbm, src, w1_buf, sem):
    head = head_out.shape[0]
    sec = lax.axis_index("section")

    @pl.when(sec == 0)
    def _():
        pltpu.make_async_copy(other_k.at[0], src.at[1], sem.at[1]).start()
        pltpu.make_async_copy(own_k.at[0], src.at[0], sem.at[0]).start()

    @pl.when(sec != 0)
    def _():
        pltpu.make_async_copy(own_k.at[0], src.at[1], sem.at[1]).start()
        pltpu.make_async_copy(other_k.at[0], src.at[0], sem.at[0]).start()

    load = pltpu.make_async_copy(x_hbm.at[sec * (x_hbm.shape[0] // 2), pl.ds(0, head)], head_out, sem.at[2])
    load.start()
    pltpu.make_async_copy(own_k.at[0], src.at[1], sem.at[1]).wait()
    lay_out(src, 1, w1_buf)
    store = pltpu.make_async_copy(w1_buf, w1_hbm, sem.at[3])
    store.start()
    pltpu.make_async_copy(own_k.at[0], src.at[0], sem.at[0]).wait()
    lay_out(src, 0, w0_out)
    load.wait()
    store.wait()


def conv_kernel(index, which, members, n_space, chunks, *refs):
    if index == 0:
        (ra_ref, rb_ref, stats_ref, own_p, other_p, head_ref, w_ref, lat_hbm,
         y_out, stats_out, ha_out, hb_out,
         xm, xr, rem_buf, z_buf, lat_buf, sem) = refs
        head = head_ref.shape[0]
        loads = []
        planes = [(xm.at[s], xr.at[s]) for s in range(2)]
    elif which == 0:
        (ra_ref, rb_ref, stats_ref, own_p, other_p, x_ref, w_hbm, lat_hbm,
         send_out, keep_out, w_ref, lat_next, xm_next, xr_next,
         xm, xr, rem_buf, z_buf, lat_buf, sem) = refs
        head = 0
        loads = [pltpu.make_async_copy(w_hbm, w_ref, sem.at[2])]
        planes = [(xm.at[0], xr.at[0]), (xm_next, xr_next)]
    else:
        (own_p, other_p, x_ref, w_ref, lat_next, xm_next, xr_next,
         send_out, keep_out,
         z_buf) = refs
        loads = []
        planes = [None, (xm_next, xr_next)]
    n, rows, cols, ch = lat_buf.shape if index == 0 else x_ref.shape
    chosen = range(n)
    padded_rows = rows + 2
    rem = ch - 256
    sec = lax.axis_index("section")
    space = lax.axis_index("space")
    even = space % 2 == 0
    if index == 0:
        for s in range(n):
            low = head if s == 0 else 0
            loads.append(
                pltpu.make_async_copy(
                    lat_hbm.at[sec * n + s, pl.ds(low, rows - low)], lat_buf.at[s, pl.ds(low, rows - low)], sem.at[s]
                )
            )
    elif which == 0:
        loads.append(pltpu.make_async_copy(lat_hbm.at[sec * n], lat_buf.at[0], sem.at[0]))
        more = pl.ds(0, MORE)
        loads.append(pltpu.make_async_copy(lat_hbm.at[sec * n + 1, more], lat_buf.at[1, more], sem.at[3]))
        next_load = pltpu.make_async_copy(lat_hbm.at[sec * n + 1], lat_next, sem.at[1])
    for cp in loads:
        cp.start()
    if index == 1 and which == 0:
        next_load.start()

    def source_row(s, r):
        if index == 1:
            return x_ref[s, r]
        if s == 0 and r < head:
            return head_ref[r]
        return lat_buf[s, r]

    params = jnp.where(sec == index, own_p[...], other_p[...])
    gain, shift, bias = params[0:1], params[1:2], params[2:3]
    if index + which < 2:
        total = stats_ref[0]
        for i in range(1, n_space):
            total = total + stats_ref[i]
        packed = []
        for s in range(n):
            mean = total[2 * s : 2 * s + 1] * (1.0 / members)
            var = jnp.maximum(total[2 * s + 1 : 2 * s + 2] * (1.0 / members) - mean * mean, 0.0)
            packed += [mean, lax.rsqrt(var + 1e-05)]
        packed = jnp.concatenate(packed + [jnp.zeros((8 - 2 * n, 128), F32)], axis=0)
        spread = exact_dot(packed, one_hot((128, ch), 1, ch // GROUPS))
        half_a = [0.5 * (spread[2 * s + 1 : 2 * s + 2] * gain) for s in range(n)]
        half_b = [0.5 * shift - spread[2 * s : 2 * s + 1] * half_a[s] for s in range(n)]

    def normalize(s, j):
        if j == 0:
            source = jnp.where(even, rb_ref[s], ra_ref[s])
        elif j == padded_rows - 1:
            source = jnp.where(even, ra_ref[s], rb_ref[s])
        else:
            source = source_row(s, j - 1)
        half = source.astype(F32) * half_a[s] + half_b[s]
        y = half + half * jnp.tanh(half)
        if j == 0:
            y = jnp.where(space == 0, 0.0, y)
        if j == padded_rows - 1:
            y = jnp.where(space == n_space - 1, 0.0, y)
        planes[s][0][pl.ds(j * cols, cols), :] = y[:, 0:256].astype(BF16)
        rem_buf[s, j] = y[:, 256:ch]
        if j >= 2:
            parts = [rem_buf[s, j - 2], rem_buf[s, j - 1], rem_buf[s, j], jnp.zeros((cols, 256 - 3 * rem), F32)]
            planes[s][1][pl.ds((j - 2) * cols, cols), :] = jnp.concatenate(parts, axis=1).astype(BF16)

    def multiply(s, r0, count, slot):
        m = count * cols
        lhs = jnp.concatenate(
            [planes[s][0][pl.ds((r0 + dr) * cols, m), :] for dr in range(3)] + [planes[s][1][pl.ds(r0 * cols, m), :]],
            axis=1,
        )
        z_buf[slot, 0:m, :] = jnp.dot(lhs, w_ref[...], preferred_element_type=F32)

    first_slab = lax.broadcasted_iota(jnp.int32, (8, 256), 0) == 0
    last_slab = lax.broadcasted_iota(jnp.int32, (8, 256), 0) == 7

    def down(z, width):
        moved = pltpu.roll(z, 1, 0)
        head = jnp.where(first_slab[:, :width], 0.0, moved[0:8])
        return jnp.concatenate([head, moved[8:]], axis=0)

    def up(z, width):
        moved = pltpu.roll(z, cols - 1, 0)
        tail = jnp.where(last_slab[:, :width], 0.0, moved[cols - 8 :])
        return jnp.concatenate([moved[: cols - 8], tail], axis=0)

    acc = [[jnp.zeros((8, ch), F32) for _ in range(2)] for _ in range(n)]

    def finish_row(s, r, slot, at):
        at = pl.ds(at * cols, cols)
        main = z_buf[slot, at, 256:512] + down(z_buf[slot, at, 0:256], 256) + up(z_buf[slot, at, 512:768], 256)
        left = z_buf[slot, at, 768:896]
        right = z_buf[slot, at, 896:1024]
        side = down(left, 128) + pltpu.roll(left, 64, 1) + up(right, 128)
        out = jnp.concatenate([main, side[:, 0:rem]], axis=1) + bias
        if index == 1:
            out = out + (lat_buf[s, r] if which == 0 else lat_next[r]).astype(F32)
        rounded = out.astype(BF16)
        if index == 0:
            y_out[s, r] = rounded
            back = rounded.astype(F32)
            acc[s][0] = acc[s][0] + fold_rows(back)
            acc[s][1] = acc[s][1] + fold_rows(back * back)
        else:
            kept = source_row(s, r)
            place = s * rows + r if which == 0 else r - MORE
            send_out[place] = jnp.where(sec == 0, rounded, kept)
            keep_out[place] = jnp.where(sec == 0, kept, rounded)

    row_a = jnp.where(even, rows - 1, 0)
    tasks = []
    for s in chosen:
        r0 = 0
        for count in chunks[s]:
            if index == 0 or (s == 0 or r0 < MORE) == (which == 0):
                tasks.append((s, r0, count))
            r0 += count
    done = [0] * n

    def prepare(task):
        s, r0, count = task
        if index + which == 2:
            return
        while done[s] < r0 + count + 2:
            normalize(s, done[s])
            done[s] += 1

    def complete(k):
        s, r0, count = tasks[k]
        for r in range(count):
            finish_row(s, r0 + r, k % 2, r)
        if index == 0 and r0 + count == rows:
            ha_out[s] = y_out[s, row_a]
            hb_out[s] = y_out[s, rows - 1 - row_a]

    early = EARLY[index + which]
    if index == 0:
        for k in range(early):
            prepare(tasks[k])
            multiply(*tasks[k], k % 2)
            if k > 0:
                complete(k - 1)
    else:
        for s in range(n) if which == 0 else ():
            for j in range(padded_rows):
                normalize(s, j)
            done[s] = padded_rows
    for cp in loads:
        cp.wait()
    for k, task in enumerate(tasks):
        if index == 0 and k < early:
            continue
        prepare(task)
        multiply(*task, k % 2)
        if k + 1 < len(tasks):
            prepare(tasks[k + 1])
        if k > 0:
            complete(k - 1)
    complete(len(tasks) - 1)
    if index == 1 and which == 0:
        next_load.wait()
    if index == 0:
        rows_out = []
        for s in range(n):
            rows_out += [v.sum(axis=0, keepdims=True) for v in acc[s]]
        sums = jnp.concatenate(rows_out + [jnp.zeros((8 - 2 * n, ch), F32)], axis=0)
        send_group_sums(sums, stats_out, ch // GROUPS)


def keep_kernel(keep_0, keep_1, received, full_out, sem):
    rows = full_out.shape[1]
    own = 2 * lax.axis_index("section")
    head, more, rest = pl.ds(0, rows), pl.ds(rows, MORE), pl.ds(MORE, rows - MORE)
    top = pl.ds(0, MORE)
    copies = [
        pltpu.make_async_copy(keep_0.at[head], full_out.at[own], sem.at[0]),
        pltpu.make_async_copy(keep_0.at[more], full_out.at[own + 1, top], sem.at[1]),
        pltpu.make_async_copy(keep_1, full_out.at[own + 1, rest], sem.at[2]),
        pltpu.make_async_copy(received.at[head], full_out.at[2 - own], sem.at[3]),
        pltpu.make_async_copy(received.at[more], full_out.at[3 - own, top], sem.at[4]),
    ]
    for cp in copies:
        cp.start()
    for cp in copies:
        cp.wait()


def finish_kernel(full_in, received, full_out, sem):
    rest = pl.ds(MORE, full_out.shape[1] - MORE)
    cp = pltpu.make_async_copy(received, full_out.at[3 - 2 * lax.axis_index("section"), rest], sem)
    cp.start()
    cp.wait()


def swap(array):
    return lax.ppermute(array, "section", [(0, 1), (1, 0)])


def on_device(latents, kernels, norm_gain, norm_bias, conv_bias):
    samples, rows, cols, ch = latents.shape
    n = samples // lax.axis_size("section")
    n_space = lax.axis_size("space")
    members = rows * n_space * cols * (ch // GROUPS)
    pairs_a = [(i, i ^ 1) for i in range(n_space)]
    pairs_b = []
    for c in range(lax.axis_size("section")):
        pairs_b += [(c * n_space + e, (1 - c) * n_space + e) for e in (0, n_space - 1)]
        pairs_b += [(c * n_space + i, c * n_space + (i - 1 if i % 2 == 0 else i + 1)) for i in range(1, n_space - 1)]
    shape = jax.ShapeDtypeStruct
    stats_shape = pltpu.VMEM((n_space, 8, 128), F32)
    edge_shape = pltpu.VMEM((n, cols, ch), BF16)
    part_shape = shape((n, rows, cols, ch), BF16)
    limit = pltpu.CompilerParams(vmem_limit_bytes=32 * 1024 * 1024)

    latents = pltpu.with_memory_space_constraint(latents, pltpu.HBM)
    kernels = pltpu.with_memory_space_constraint(kernels, pltpu.HBM)
    own_p = jnp.concatenate([norm_gain, norm_bias, conv_bias], axis=0)
    other_p = swap(own_p)
    other_k = pltpu.with_memory_space_constraint(swap(kernels), pltpu.HBM)

    stats, ha, hb = pl.pallas_call(
        stats_kernel,
        out_shape=(stats_shape, edge_shape, edge_shape),
        in_specs=[HBM],
        out_specs=(VM, VM, VM),
        scratch_shapes=[
            pltpu.VMEM((n, rows, cols, ch), BF16),
            pltpu.SemaphoreType.DMA((n,)),
        ],
        compiler_params=limit,
        name="stats",
    )(latents)
    ra = lax.ppermute(ha, "space", pairs_a)
    rb = lax.ppermute(hb, ("section", "space"), pairs_b)
    stats = lax.all_to_all(stats, "space", split_axis=0, concat_axis=0, tiled=True)

    head = HEAD
    w_type = (1024, 1024)

    head_ref, w0, w1 = pl.pallas_call(
        prepare_kernel,
        out_shape=(pltpu.VMEM((head, cols, ch), BF16), pltpu.VMEM(w_type, BF16), pltpu.HBM(w_type, BF16)),
        in_specs=[HBM, HBM, HBM],
        out_specs=(VM, VM, HBM),
        scratch_shapes=[
            pltpu.VMEM((2, *kernels.shape[1:]), BF16),
            pltpu.VMEM(w_type, BF16),
            pltpu.SemaphoreType.DMA((4,)),
        ],
        compiler_params=pltpu.CompilerParams(vmem_limit_bytes=16 * 1024 * 1024),
        name="prepare",
    )(latents, kernels, other_k)
    w1 = pltpu.with_memory_space_constraint(w1, pltpu.HBM)

    chunks = CHUNKS
    most = max(max(c) for c in chunks)

    def conv(index, which, operands, out_shape):
        body = lambda *refs: conv_kernel(index, which, members, n_space, chunks, *refs)
        in_hbm = (1, 2, 0)[index + which]
        z_type = pltpu.VMEM((2, most * cols, 1024), F32)
        if index + which < 2:
            held = n if index == 0 else 1
            scratch = [
                pltpu.VMEM((held, (rows + 2) * cols, 256), BF16),
                pltpu.VMEM((held, rows * cols, 256), BF16),
                pltpu.VMEM((n, rows + 2, cols, ch - 256), F32),
                z_type,
                pltpu.VMEM((n, rows, cols, ch), BF16),
                pltpu.SemaphoreType.DMA((4,)),
            ]
        else:
            scratch = [z_type]
        return pl.pallas_call(
            body,
            out_shape=out_shape,
            in_specs=[VM] * (len(operands) - in_hbm) + [HBM] * in_hbm,
            out_specs=(VM,) * len(out_shape),
            scratch_shapes=scratch,
            compiler_params=limit,
            name="conv%d%d" % (index, which),
        )(*operands)

    first, stats, ha, hb = conv(
        0,
        0,
        (ra, rb, stats, own_p, other_p, head_ref, w0, latents),
        (pltpu.VMEM(part_shape.shape, BF16), stats_shape, edge_shape, edge_shape),
    )
    ra = lax.ppermute(ha, "space", pairs_a)
    rb = lax.ppermute(hb, ("section", "space"), pairs_b)
    stats = lax.all_to_all(stats, "space", split_axis=0, concat_axis=0, tiled=True)
    full_shape = shape((samples, rows, cols, ch), BF16)
    common = (ra, rb, stats, own_p, other_p, first)
    sample_shape = pltpu.VMEM((rows, cols, ch), BF16)
    large = pltpu.VMEM((rows + MORE, cols, ch), BF16)
    little = pltpu.VMEM((rows - MORE, cols, ch), BF16)
    plane_shapes = (pltpu.VMEM(((rows + 2) * cols, 256), BF16), pltpu.VMEM((rows * cols, 256), BF16))
    send_0, keep_0, *rest = conv(
        1,
        0,
        (*common, w1, latents),
        (large, large, pltpu.VMEM(w_type, BF16), sample_shape, *plane_shapes),
    )
    received_0 = swap(send_0)
    send_1, keep_1 = conv(1, 1, (own_p, other_p, first, *rest), (little, little))
    received_1 = swap(send_1)
    small = pltpu.CompilerParams(vmem_limit_bytes=1024 * 1024)
    full = pl.pallas_call(
        keep_kernel,
        out_shape=full_shape,
        in_specs=[VM, VM, VM],
        out_specs=HBM,
        scratch_shapes=[pltpu.SemaphoreType.DMA((5,))],
        compiler_params=small,
        name="keep",
    )(keep_0, keep_1, received_0)
    full = pl.pallas_call(
        finish_kernel,
        out_shape=full_shape,
        in_specs=[HBM, VM],
        out_specs=HBM,
        scratch_shapes=[pltpu.SemaphoreType.DMA],
        input_output_aliases={0: 0},
        compiler_params=small,
        name="finish",
    )(full, received_1)
    return full[None]


def solution(mesh):
    return jax.shard_map(
        on_device,
        mesh=mesh,
        in_specs=(
            P("dp", "space", None, None),
            P("section", None, None, None, None),
            P("section", None),
            P("section", None),
            P("section", None),
        ),
        out_specs=P("section", "dp", "space", None, None),
        check_vma=False,
    )
```
